32 devices in a mesh: seq: 8 (over z, x), head: 4 (over y, core).
Axes of the slice: x: 2, y: 2, z: 4, core: 2. Of those that a mesh axis runs over, the one named last changes fastest.
Arguments:
- queries: bfloat16 [8192, 1536], P('seq', 'head'), may hold values from -5 to 5
- key_vectors: bfloat16 [8192, 1536], P('seq', 'head'), may hold values from -5 to 5
- value_vectors: bfloat16 [8192, 1536], P('seq', 'head'), may hold values from -6 to 6
- out_grad: bfloat16 [8192, 1536], P('seq', 'head'), may hold values from -6 to 6
- gate_logit: float32 [12], P('head'), may hold values from -2 to 2
- doc_index: int32 [8], replicated, may hold values from 0 to 3, never falling along the last dimension, each value on 1 to 4 neighbouring positions
Outputs:
- query_grad: float32 [8192, 1536], P('seq', 'head')
- key_grad: float32 [8192, 1536], P('seq', 'head')
- value_grad: float32 [8192, 1536], P('seq', 'head')
- gate_grad: float32 [12], P('head')
The draws below stay inside these ranges and needn't reach their ends.
Inputs may be any that keep to these rules, and one draw needn't show every extreme that they name: `doc_index`: never falls from one segment to the next; every document holds 1 to 4 segments, and one holds exactly 4.
All inputs are finite; a program needn't handle non-finite values.
Results may differ from the reference program's by a relative error of at most 0.0017.
The reference program's roundings to bfloat16 on the way (of `attention_low` and `score_grad`) count: a program that leaves them out, or rounds other values in their place, can miss the bound.
Values sent between devices are 32-bit elements; how exact they have to be, the bound alone decides.
A program may use at most 128 MiB of HBM per device.

```python
import math
import jax
import jax.numpy as jnp
import numpy as np
from jax import lax

H = 12
HD = 128
TOK_DEV = 1024
DOCS = 4
SHARDS = 8
TOKENS = 8192


def paired(base_key):
    grid_shape = (TOKENS, H * HD)
    first_key, second_key, scale_key, other_scale, sign_key, noise_key = jax.random.split(base_key, 6)
    query_draw = jax.random.truncated_normal(first_key, -5.0, 5.0, grid_shape, jnp.float32)
    key_draw = jax.random.truncated_normal(second_key, -5.0, 5.0, grid_shape, jnp.float32)
    noise = jax.random.normal(noise_key, grid_shape, jnp.float32)
    value_draw = jnp.clip(1.8 * key_draw + 0.6 * noise, -6.0, 6.0)
    return (query_draw, key_draw, value_draw)


def draw_queries(key, part):
    return paired(jax.random.fold_in(key, 11))[0].astype(jnp.bfloat16)


def draw_key_vectors(key, part):
    return paired(jax.random.fold_in(key, 11))[1].astype(jnp.bfloat16)


def draw_value_vectors(key, part):
    return paired(jax.random.fold_in(key, 11))[2].astype(jnp.bfloat16)


def level_of(own_key, shape, pieces, least, largest):
    factor_of, own = 1.0, jax.random.fold_in(own_key, 6)
    for axis_at, parts in pieces:
        draws = jnp.exp(jax.random.uniform(jax.random.fold_in(own, axis_at), (parts,), jnp.float32, least / len(pieces), largest / len(pieces)))
        factor_of = factor_of * jnp.repeat(draws, shape[axis_at] // parts).reshape([-1 if axis == axis_at else 1 for axis in range(len(shape))])
    return factor_of


def profile(number_of, total, bound, slope):
    loads = [(1 << 20) // math.isqrt(standing ** slope) + 1 for standing in range(2, number_of + 1)]
    rest, given = total - bound - (number_of - 1), [1] * (number_of - 1)
    while rest > 0:
        free = [i for i in range(number_of - 1) if given[i] < bound]
        pool, remaining = sum([loads[i] for i in free]), rest
        for i in free:
            more = min(bound - given[i], max(1, remaining * loads[i] // pool), rest)
            given[i] = given[i] + more
            rest = rest - more
    return np.array([bound] + given)


def ragged(stream_key, amount, total, bound, lean):
    if amount == 2:
        one = jax.random.randint(stream_key, (), max(1, total - bound), min(bound, total - 1) + 1)
        return jnp.stack([one, total - one])
    sizes = jnp.asarray(profile(amount, total, bound, lean), jnp.int32)
    couples = (amount - 1) // 2
    giver, sink = sizes[1:1 + 2 * couples:2], sizes[2:2 + 2 * couples:2]
    slack = jnp.minimum(giver - 1, bound - sink)
    passed = jax.random.randint(jax.random.fold_in(stream_key, 1), (couples,), 0, 1 << 20) % (slack + 1)
    sizes = sizes.at[1:1 + 2 * couples:2].set(giver - passed).at[2:2 + 2 * couples:2].set(sink + passed)
    return sizes[jax.random.permutation(jax.random.fold_in(stream_key, 2), amount)]


def centred(rng, dims, deviation, reach, cuts=(), held_as=jnp.bfloat16):
    result = deviation * jax.random.normal(rng, dims, jnp.float32)
    if cuts:
        result = result * level_of(rng, dims, cuts, -0.22, 0.18)
    return jnp.clip(result, -reach, reach).astype(held_as)


def setup_inputs(seed: int = 0) -> dict:
    seeds = jax.random.split(jax.random.key(seed), 7)
    return {
        "queries": draw_queries(jax.random.fold_in(seeds[6], 71), 0),
        "key_vectors": draw_key_vectors(jax.random.fold_in(seeds[6], 71), 0),
        "value_vectors": draw_value_vectors(jax.random.fold_in(seeds[6], 71), 0),
        "out_grad": centred(seeds[3], (TOKENS, H * HD), 1.0, 6.0, ((0, 8), (1, 4))),
        "gate_logit": jnp.clip(jax.random.uniform(seeds[4], (H,), jnp.float32, -2.0, 2.0) * level_of(seeds[4], (H,), ((0, 4),), -0.4, 0.0), -2.0, 2.0),
        "doc_index": jnp.searchsorted(jnp.cumsum(ragged(seeds[5], DOCS, SHARDS, SHARDS // 2, 2)), jnp.arange(SHARDS), side="right").astype(jnp.int32),
    }


def feature(values_in):
    return jnp.where(values_in > 0, values_in + 1.0, jnp.exp(jnp.minimum(values_in, 0.0)))


def feature_slope(values_in):
    return jnp.where(values_in > 0, 1.0, jnp.exp(jnp.minimum(values_in, 0.0)))


def contribution(key_vectors, value_vectors, head_count):
    row_count = key_vectors.shape[0]
    key_feature = feature(key_vectors.astype(jnp.float32)).astype(jnp.bfloat16)
    feature_three = key_feature.reshape(row_count, head_count, -1).astype(jnp.float32)
    value_three = value_vectors.reshape(row_count, head_count, -1).astype(jnp.float32)
    memory_part = jnp.einsum("nhd,nhe->hde", feature_three, value_three, precision=lax.Precision.HIGHEST)
    norm_part = jnp.sum(feature_three, axis=0)
    return memory_part, norm_part, key_feature


def head_work(head_index, queries, key_vectors, value_vectors, out_grad, query_feature, memory_prev, norm_prev, gate_prob):
    head_size = memory_prev.shape[-1]
    row_count = queries.shape[0]

    def take_columns(matrix):
        return lax.dynamic_slice_in_dim(matrix, head_index * head_size, head_size, 1)

    query_head = take_columns(queries)
    key_head = take_columns(key_vectors)
    value_head = take_columns(value_vectors)
    grad_head = take_columns(out_grad)
    query_float = take_columns(query_feature).astype(jnp.float32)
    memory_share = gate_prob[head_index]
    local_share = 1.0 - memory_share
    score_scale = head_size ** -0.5
    scores = lax.dot_general(query_head, key_head, (((1,), (1,)), ((), ())), preferred_element_type=jnp.float32) * score_scale
    row_ids = lax.broadcasted_iota(jnp.int32, (row_count, row_count), 0)
    col_ids = lax.broadcasted_iota(jnp.int32, (row_count, row_count), 1)
    scores = jnp.where(row_ids >= col_ids, scores, -1e30)
    attention = jnp.exp(scores - jnp.max(scores, axis=1, keepdims=True))
    attention = attention / jnp.sum(attention, axis=1, keepdims=True)
    attention_low = attention.astype(jnp.bfloat16)
    local_read = jnp.dot(attention_low, value_head, preferred_element_type=jnp.float32)
    prob_grad = local_share * lax.dot_general(grad_head, value_head, (((1,), (1,)), ((), ())), preferred_element_type=jnp.float32)
    row_delta = jnp.sum(prob_grad * attention, axis=1, keepdims=True)
    score_grad = (attention * (prob_grad - row_delta)).astype(jnp.bfloat16)
    query_local = jnp.dot(score_grad, key_head, preferred_element_type=jnp.float32) * score_scale
    key_local = lax.dot_general(score_grad, query_head, (((0,), (0,)), ((), ())), preferred_element_type=jnp.float32) * score_scale
    value_local = local_share * lax.dot_general(attention_low, grad_head, (((0,), (0,)), ((), ())), preferred_element_type=jnp.float32)
    memory_head = memory_prev[head_index]
    norm_head = norm_prev[head_index]
    numerator = jnp.dot(query_float, memory_head, precision=lax.Precision.HIGHEST)
    denominator = 1.0 + jnp.dot(query_float, norm_head, precision=lax.Precision.HIGHEST)
    memory_read = numerator / denominator[:, None]
    grad_float = grad_head.astype(jnp.float32)
    num_grad = memory_share * grad_float / denominator[:, None]
    den_grad = -memory_share * jnp.sum(grad_float * memory_read, axis=1) / denominator
    grad_memory = lax.dot_general(query_float, num_grad, (((0,), (0,)), ((), ())), precision=lax.Precision.HIGHEST)
    grad_norm = jnp.dot(den_grad, query_float, precision=lax.Precision.HIGHEST)
    feature_grad = lax.dot_general(num_grad, memory_head, (((1,), (1,)), ((), ())), precision=lax.Precision.HIGHEST) + den_grad[:, None] * norm_head[None, :]
    query_grad = query_local + feature_grad * feature_slope(query_head.astype(jnp.float32))
    gate_part = memory_share * local_share * jnp.sum(grad_float * (memory_read - local_read))
    return query_grad, key_local, value_local, grad_memory, grad_norm, gate_part


def to_rows(stacked):
    return jnp.transpose(stacked, (1, 0, 2)).reshape(stacked.shape[1], -1)


def shard_work(queries, key_vectors, value_vectors, out_grad, memory_prev, norm_prev, gate_prob):
    query_feature = feature(queries.astype(jnp.float32)).astype(jnp.bfloat16)

    def one_head(head_index):
        return head_work(head_index, queries, key_vectors, value_vectors, out_grad, query_feature, memory_prev, norm_prev, gate_prob)

    results = lax.map(one_head, jnp.arange(gate_prob.shape[0], dtype=jnp.int32))
    return to_rows(results[0]), to_rows(results[1]), to_rows(results[2]), results[3], results[4], results[5]


def finish(key_vectors, value_vectors, key_feature, key_local, value_local, later_memory, later_norm):
    row_count = key_vectors.shape[0]
    head_count = later_memory.shape[0]
    value_three = value_vectors.reshape(row_count, head_count, -1).astype(jnp.float32)
    feature_three = key_feature.reshape(row_count, head_count, -1).astype(jnp.float32)
    key_three = key_vectors.reshape(row_count, head_count, -1).astype(jnp.float32)
    feature_grad = jnp.einsum("nhe,hde->nhd", value_three, later_memory, precision=lax.Precision.HIGHEST) + later_norm[None]
    key_grad = key_local + (feature_grad * feature_slope(key_three)).reshape(row_count, -1)
    value_extra = jnp.einsum("nhd,hde->nhe", feature_three, later_memory, precision=lax.Precision.HIGHEST)
    value_grad = value_local + value_extra.reshape(row_count, -1)
    return key_grad, value_grad


def reference(queries, key_vectors, value_vectors, out_grad, gate_logit, doc_index):
    width = H * HD

    def by_shard(matrix):
        return matrix.reshape(SHARDS, TOK_DEV, width)

    query_shards = by_shard(queries)
    key_shards = by_shard(key_vectors)
    value_shards = by_shard(value_vectors)
    grad_shards = by_shard(out_grad)
    gate_prob = jax.nn.sigmoid(gate_logit)
    memory_part, norm_part, key_feature = lax.map(lambda packed: contribution(packed[0], packed[1], H), (key_shards, value_shards))
    opening = jnp.concatenate([jnp.ones((1,), jnp.bool_), doc_index[1:] != doc_index[:-1]])
    closing = jnp.concatenate([doc_index[:-1] != doc_index[1:], jnp.ones((1,), jnp.bool_)])
    start_state = (jnp.zeros((H, HD, HD), jnp.float32), jnp.zeros((H, HD), jnp.float32))

    def forward_step(totals, packed):
        memory_before = jnp.where(packed[2], 0.0, totals[0])
        norm_before = jnp.where(packed[2], 0.0, totals[1])
        return (memory_before + packed[0], norm_before + packed[1]), (memory_before, norm_before)

    final_state, prev_state = lax.scan(forward_step, start_state, (memory_part, norm_part, opening))
    memory_prev, norm_prev = prev_state

    def run_shard(packed):
        return shard_work(packed[0], packed[1], packed[2], packed[3], packed[4], packed[5], gate_prob)

    query_grad, key_local, value_local, grad_memory, grad_norm, gate_parts = lax.map(run_shard, (query_shards, key_shards, value_shards, grad_shards, memory_prev, norm_prev))

    def backward_step(totals, packed):
        memory_after = jnp.where(packed[2], 0.0, totals[0])
        norm_after = jnp.where(packed[2], 0.0, totals[1])
        return (memory_after + packed[0], norm_after + packed[1]), (memory_after, norm_after)

    back_state, later_state = lax.scan(backward_step, start_state, (grad_memory, grad_norm, closing), reverse=True)
    later_memory, later_norm = later_state

    def run_finish(packed):
        return finish(packed[0], packed[1], packed[2], packed[3], packed[4], packed[5], packed[6])

    key_grad, value_grad = lax.map(run_finish, (key_shards, value_shards, key_feature, key_local, value_local, later_memory, later_norm))
    gate_grad = jnp.sum(gate_parts, axis=0)
    return query_grad.reshape(TOKENS, width), key_grad.reshape(TOKENS, width), value_grad.reshape(TOKENS, width), gate_grad
```

```python
import functools
import math

import jax
import jax.numpy as jnp
from jax import lax
from jax.experimental import pallas as pl
from jax.experimental.pallas import tpu as pltpu
from jax.sharding import PartitionSpec as P

MESH = pl.DeviceIdType.MESH
F32 = jnp.float32
BF16 = jnp.bfloat16


def slope(x):
    return jnp.exp(jnp.minimum(x, 0.0))


def dot_nn(a, b):
    return lax.dot_general(a, b, (((1,), (0,)), ((), ())), preferred_element_type=F32)


def dot_nt(a, b):
    return lax.dot_general(a, b, (((1,), (1,)), ((), ())), preferred_element_type=F32)


def dot_tn(a, b):
    return lax.dot_general(a, b, (((0,), (0,)), ((), ())), preferred_element_type=F32)


def split(x):
    high = x.astype(BF16)
    return high, (x - high.astype(F32)).astype(BF16)


def merged(*lists):
    order = []
    for which, items in enumerate(lists):
        for at, item in enumerate(items):
            order.append(((at + 0.5) / len(items), which, at, item))
    return [entry[3] for entry in sorted(order, key=lambda entry: entry[:3])]


def kernel(
    n, steps, reach, heads, size, block,
    doc_hbm, logit_hbm, q_hbm, k_hbm, v_hbm, g_hbm,
    qo, ko, vo, gate_o,
    doc_ref, logit_ref, q_ref, k_ref, v_ref, g_ref, load_sem,
    kf, qf, k_slope, q_slope, inv_den, s_buf, g_buf, k_turned, gate_rows, gate_all,
    norm_src, norm_got, norm_sum, mem_src, mem_got, mem_sum,
    norm_send, norm_recv, mem_send, mem_recv, gate_send, gate_recv, entered,
):
    me = lax.axis_index("seq")
    rows = q_ref.shape[0]
    blocks = rows // block
    scale = size ** -0.5
    factor = scale * math.log2(math.e)
    signs = (1, -1)
    barrier = pltpu.get_barrier_semaphore()
    loads = [
        pltpu.make_async_copy(source, target, load_sem.at[i])
        for i, (source, target) in enumerate((
            (k_hbm, k_ref), (v_hbm, v_ref), (q_hbm, q_ref), (g_hbm, g_ref),
            (doc_hbm, doc_ref), (logit_hbm, logit_ref),
        ))
    ]
    for i in (0, 4, 5, 1, 2, 3):
        loads[i].start()

    def peer(way, dist):
        return {"seq": lax.rem(me + signs[way] * dist + n, n)}

    def can_send(way, dist):
        return me + dist < n if way == 0 else me >= dist

    def can_recv(way, dist):
        return me >= dist if way == 0 else me + dist < n

    for dist in range(1, reach + 1):
        for way in range(2):
            @pl.when(can_send(way, dist))
            def _():
                pl.semaphore_signal(barrier, inc=1, device_id=peer(way, dist), device_id_type=MESH)

    def cols(h):
        return slice(h * size, (h + 1) * size)

    def part(i):
        return slice(i * block, (i + 1) * block)

    def share(h, width):
        return 1.0 / (1.0 + jnp.exp(-jnp.full((1, width), logit_ref[h], F32)))

    def weight(way, dist):
        other = lax.rem(me - signs[way] * dist + n, n)
        return jnp.where(doc_ref[other] == doc_ref[me], 1.0, 0.0).astype(F32)

    def norm_copy(way, dist):
        return pltpu.make_async_remote_copy(
            src_ref=norm_src.at[way], dst_ref=norm_got.at[way, dist - 1],
            send_sem=norm_send.at[way, dist - 1], recv_sem=norm_recv.at[way, dist - 1],
            device_id=peer(way, dist), device_id_type=MESH,
        )

    def mem_copy(way, step, h):
        return pltpu.make_async_remote_copy(
            src_ref=mem_src.at[way, step, h], dst_ref=mem_got.at[way, step, h],
            send_sem=mem_send.at[way, step, h], recv_sem=mem_recv.at[way, step, h],
            device_id=peer(way, 1 << step), device_id_type=MESH,
        )

    def gate_copy(other):
        return pltpu.make_async_remote_copy(
            src_ref=gate_rows, dst_ref=gate_all.at[me],
            send_sem=gate_send.at[other - 1], recv_sem=gate_recv.at[other - 1],
            device_id={"seq": lax.rem(me + other, n)}, device_id_type=MESH,
        )

    def tell(turn):
        for way in range(2):
            @pl.when(can_send(way, reach))
            def _():
                pl.semaphore_signal(entered.at[turn, way], inc=1, device_id=peer(way, reach), device_id_type=MESH)

    def hear(turn):
        for way in range(2):
            @pl.when(can_recv(way, reach))
            def _():
                pl.semaphore_wait(entered.at[turn, way], 1)

    def send_norms(way):
        for dist in range(1, reach + 1):
            @pl.when(can_send(way, dist))
            def _():
                norm_copy(way, dist).start()

    def take_norms(way):
        norm_sum[way] = jnp.zeros_like(norm_sum[way])
        for dist in range(1, reach + 1):
            @pl.when(can_recv(way, dist))
            def _():
                norm_copy(way, dist).wait_recv()
                norm_sum[way] += weight(way, dist) * norm_got[way, dist - 1]

    def send_mem(way, step, h):
        @pl.when(can_send(way, 1 << step))
        def _():
            mem_copy(way, step, h).start()

    def take_mem(way, step, h):
        if step == 0:
            mem_sum[way, h] = jnp.zeros_like(mem_sum[way, h])

        @pl.when(can_recv(way, 1 << step))
        def _():
            mem_copy(way, step, h).wait_recv()
            mem_sum[way, h] += weight(way, 1 << step) * mem_got[way, step, h]

        if step + 1 < steps:
            mem_src[way, step + 1, h] = mem_src[way, 0, h] + mem_sum[way, h]
            send_mem(way, step + 1, h)

    units = [(h, i) for h in range(heads) for i in range(blocks)]
    kept = [{} for _ in units]

    def scores(u):
        h, i = units[u]
        held = s_buf.at[u % 3]

        def tile(j):
            def run():
                if i == 0:
                    k_turned[h] = k_ref[:, cols(h)].T
                out = dot_nt(k_ref[part(j), cols(h)], q_ref[part(i), cols(h)])
                if j == i:
                    key_ids = lax.broadcasted_iota(jnp.int32, (block, block), 0)
                    query_ids = lax.broadcasted_iota(jnp.int32, (block, block), 1)
                    out = jnp.where(key_ids <= query_ids, out, -1e30)
                held[part(j), :] = out
                top = jnp.max(out, axis=0, keepdims=True)
                kept[u]["top"] = top if j == 0 else jnp.maximum(kept[u]["top"], top)
            return run

        return [tile(j) for j in range(i + 1)]

    def weights(u):
        h, i = units[u]
        held = s_buf.at[u % 3]
        grads = g_buf.at[u % 2]

        def raise_tile(j):
            def run():
                out = jnp.exp2((held[part(j), :] - kept[u]["top"]) * factor)
                held[part(j), :] = out
                total = jnp.sum(out, axis=0, keepdims=True)
                kept[u]["total"] = total if j == 0 else kept[u]["total"] + total
                if j == i:
                    kept[u]["inverse"] = 1.0 / kept[u]["total"]
            return run

        def grad_tile(j):
            def run():
                g_i = g_ref[part(i), cols(h)]
                grad = dot_nt(v_ref[part(j), cols(h)], g_i)
                grads[part(j), :] = grad
                out = held[part(j), :]
                low = (out * kept[u]["inverse"]).astype(BF16)
                delta = jnp.sum(grad * out, axis=0, keepdims=True)
                kept[u]["delta"] = delta if j == 0 else kept[u]["delta"] + delta
                piece = dot_nn(low, g_i)
                if j == i:
                    vo[part(j), cols(h)] = piece
                    kept[u]["delta"] = kept[u]["delta"] * kept[u]["inverse"]
                    kept[u]["scaled"] = kept[u]["inverse"] * (1.0 - share(h, block))
                else:
                    vo[part(j), cols(h)] += piece
            return run

        return [raise_tile(j) for j in range(i + 1)] + [grad_tile(j) for j in range(i + 1)]

    def grads(u):
        h, i = units[u]
        held = s_buf.at[u % 3]
        grads = g_buf.at[u % 2]

        def tile(j):
            def run():
                q_i = q_ref[part(i), cols(h)]
                score = held[part(j), :] * ((grads[part(j), :] - kept[u]["delta"]) * kept[u]["scaled"])
                score = score.astype(BF16)
                piece = dot_nn(score, q_i)
                if j == i:
                    ko[part(j), cols(h)] = piece
                else:
                    ko[part(j), cols(h)] += piece
                turned = dot_nn(k_turned[h, :, part(j)], score)
                kept[u]["turned"] = turned if j == 0 else kept[u]["turned"] + turned
                if j == i:
                    qo[part(i), cols(h)] = kept[u]["turned"].T * scale
            return run

        return [tile(j) for j in range(i + 1)]

    def attend(at):
        lists = []
        if 0 <= at - 2 < len(units):
            lists.append(grads(at - 2))
        if 0 <= at - 1 < len(units):
            lists.append(weights(at - 1))
        if at < len(units):
            lists.append(scores(at))
        for run in merged(*lists):
            run()

    def memory_grads():
        take_norms(0)
        for h in range(heads):
            hs = cols(h)
            norm = norm_sum[0, h:h + 1, :]
            both = jnp.zeros((size, 2 * size), F32)
            for i in range(blocks):
                low = qf[part(i), hs]
                den = 1.0 + jnp.sum(low.astype(F32) * norm, axis=1, keepdims=True)
                inv = jnp.broadcast_to(1.0 / den, (block, size))
                inv_den[h, part(i), :] = inv
                num = g_ref[part(i), hs].astype(F32) * inv
                both = both + dot_tn(low, jnp.concatenate(split(num), axis=1))
            mem_src[1, 0, h] = (both[:, :size] + both[:, size:]) * share(h, size)
            send_mem(1, 0, h)

    def read_memory(h):
        hs = cols(h)
        memory_share = share(h, size)
        norm = norm_sum[0, h:h + 1, :]
        memory = mem_sum[0, h]
        beside = jnp.concatenate(split(memory), axis=1)
        grad_norm = jnp.zeros((1, size), F32)
        for i in range(blocks):
            low = qf[part(i), hs].astype(F32)
            g_i = g_ref[part(i), hs]
            inv = inv_den[h, part(i), :]
            weighted = inv * memory_share
            turned = dot_nt(jnp.concatenate([g_i, g_i], axis=1), beside)
            product = jnp.sum(low * turned, axis=1, keepdims=True)
            den_grad = -(weighted * inv) * product
            grad_norm = grad_norm + jnp.sum(den_grad * low, axis=0, keepdims=True)
            qo[part(i), hs] += (turned * weighted + den_grad * norm) * q_slope[part(i), hs]
        norm_src[1, h:h + 1, :] = grad_norm
        row = jnp.sum(memory * mem_src[1, 0, h], axis=0, keepdims=True)
        gate_rows[h:h + 1, :] += row * (1.0 - memory_share)

    def local_gate(h):
        memory_share = share(h, size)
        row = jnp.zeros((1, size), F32)
        for i in range(blocks):
            row = row + jnp.sum(v_ref[part(i), cols(h)].astype(F32) * vo[part(i), cols(h)], axis=0, keepdims=True)
        gate_rows[h:h + 1, :] = -row * (memory_share * (1.0 - memory_share))

    def finish(h):
        hs = cols(h)
        local_share = 1.0 - share(h, size)
        high, rest = split(mem_sum[1, h])
        beside = jnp.concatenate([high, rest], axis=1)
        below = jnp.concatenate([high, rest], axis=0)
        for i in range(blocks):
            v_i = v_ref[part(i), hs]
            low = kf[part(i), hs]
            extra = dot_nt(jnp.concatenate([v_i, v_i], axis=1), beside)
            ko[part(i), hs] = ko[part(i), hs] * scale + extra * k_slope[part(i), hs]
            value = dot_nn(jnp.concatenate([low, low], axis=1), below)
            vo[part(i), hs] = vo[part(i), hs] * local_share + value

    gate_rows[...] = jnp.zeros_like(gate_rows)
    norm_src[...] = jnp.zeros_like(norm_src)
    loads[0].wait()
    for h in range(heads):
        norm = jnp.zeros((1, size), F32)
        for i in range(blocks):
            x = k_ref[part(i), cols(h)].astype(F32)
            flat = slope(x)
            k_slope[part(i), cols(h)] = flat
            low = (jnp.maximum(x, 0.0) + flat).astype(BF16)
            kf[part(i), cols(h)] = low
            norm = norm + jnp.sum(low.astype(F32), axis=0, keepdims=True)
        norm_src[0, h:h + 1, :] = norm
    for i in (4, 5, 1):
        loads[i].wait()
    for h in range(heads):
        mem_src[0, 0, h] = dot_tn(kf[:, cols(h)], v_ref[:, cols(h)])
    loads[2].wait()
    loads[3].wait()
    for h in range(heads):
        for i in range(blocks):
            x = q_ref[part(i), cols(h)].astype(F32)
            flat = slope(x)
            q_slope[part(i), cols(h)] = flat
            qf[part(i), cols(h)] = (jnp.maximum(x, 0.0) + flat).astype(BF16)
    pl.semaphore_wait(barrier, jnp.minimum(me, reach) + jnp.minimum(n - 1 - me, reach))
    send_norms(0)
    for h in range(heads):
        send_mem(0, 0, h)
    turns = -(-(n - 1) // reach) - 1
    if turns:
        tell(0)

    last = len(units) + 1
    polls = {}
    if steps > 1:
        order = [(0, 0), (0, 1), (1, 0), (0, 2), (1, 1), (1, 2)]
        order += [(way, h) for h in range(3, heads) for way in range(2)]
        order = [(way, h) for way, h in order if h < heads]
        for (way, h), at in zip(order, [4, 6, 7, 8, 9, 11] + [last] * len(order)):
            polls.setdefault(min(at, last), []).append((way, h))
    for at in range(last + 1):
        attend(at)
        if at == min(2, last):
            memory_grads()
        for way, h in polls.get(at, []):
            take_mem(way, 0, h)
        for turn in range(turns):
            if at == min(8 + 3 * turn, last):
                hear(turn)
                if turn + 1 < turns:
                    tell(turn + 1)
    for step in range(1, steps - 1):
        for h in range(heads):
            for way in range(2):
                take_mem(way, step, h)
    for h in range(heads):
        local_gate(h)
    for h in range(heads):
        take_mem(0, steps - 1, h)
        read_memory(h)
    send_norms(1)
    for other in range(1, n):
        gate_copy(other).start()
    gate_all[me] = gate_rows[...]
    for h in range(heads):
        take_mem(1, steps - 1, h)
        finish(h)
    take_norms(1)
    for h in range(heads):
        norm = norm_sum[1, h:h + 1, :]
        for i in range(blocks):
            ko[part(i), cols(h)] += norm * k_slope[part(i), cols(h)]
    for other in range(1, n):
        gate_copy(other).wait_recv()
    gates = gate_all[0]
    for other in range(1, n):
        gates = gates + gate_all[other]
    gate_o[...] = gates

    for other in range(1, n):
        gate_copy(other).wait_send()
    for way in range(2):
        for dist in range(1, reach + 1):
            @pl.when(can_send(way, dist))
            def _():
                norm_copy(way, dist).wait_send()
        for step in range(steps):
            @pl.when(can_send(way, 1 << step))
            def _():
                for h in range(heads):
                    mem_copy(way, step, h).wait_send()


def write(heads, q_ref, k_ref, v_ref, gate_ref, q_hbm, k_hbm, v_hbm, gate_o, sems):
    copies = [
        pltpu.make_async_copy(source, target, sems.at[i])
        for i, (source, target) in enumerate(((q_ref, q_hbm), (k_ref, k_hbm), (v_ref, v_hbm)))
    ]
    for copy in copies:
        copy.start()
    for h in range(heads):
        gate_o[h] = jnp.sum(gate_ref[h:h + 1, :])
    for copy in copies:
        copy.wait()


def solution(mesh):
    n = mesh.shape["seq"]
    longest = max(n // 2, 2)
    steps = (longest - 1).bit_length()
    reach = longest - 1

    def per_device(queries, key_vectors, value_vectors, out_grad, gate_logit, doc_index):
        rows, width = queries.shape
        heads = gate_logit.shape[0]
        size = width // heads
        block = min(256, rows)
        wide = jax.ShapeDtypeStruct((rows, width), F32)
        vmem = pl.BlockSpec(memory_space=pltpu.VMEM)
        smem = pl.BlockSpec(memory_space=pltpu.SMEM)
        hbm = pl.BlockSpec(memory_space=pltpu.HBM)
        tall = -(-heads // 8) * 8
        dma = pltpu.SemaphoreType.DMA
        local = pl.pallas_call(
            functools.partial(kernel, n, steps, reach, heads, size, block),
            out_shape=(wide, wide, wide, jax.ShapeDtypeStruct((tall, size), F32)),
            in_specs=[hbm] * 6,
            out_specs=(vmem,) * 4,
            scratch_shapes=[
                pltpu.SMEM(doc_index.shape, jnp.int32),
                pltpu.SMEM(gate_logit.shape, F32),
                pltpu.VMEM((rows, width), BF16),
                pltpu.VMEM((rows, width), BF16),
                pltpu.VMEM((rows, width), BF16),
                pltpu.VMEM((rows, width), BF16),
                dma((6,)),
                pltpu.VMEM((rows, width), BF16),
                pltpu.VMEM((rows, width), BF16),
                pltpu.VMEM((rows, width), F32),
                pltpu.VMEM((rows, width), F32),
                pltpu.VMEM((heads, rows, size), F32),
                pltpu.VMEM((3, rows, block), F32),
                pltpu.VMEM((2, rows, block), F32),
                pltpu.VMEM((heads, size, rows), BF16),
                pltpu.VMEM((tall, size), F32),
                pltpu.VMEM((n, tall, size), F32),
                pltpu.VMEM((2, tall, size), F32),
                pltpu.VMEM((2, reach, tall, size), F32),
                pltpu.VMEM((2, tall, size), F32),
                pltpu.VMEM((2, steps, heads, size, size), F32),
                pltpu.VMEM((2, steps, heads, size, size), F32),
                pltpu.VMEM((2, heads, size, size), F32),
                dma((2, reach)),
                dma((2, reach)),
                dma((2, steps, heads)),
                dma((2, steps, heads)),
                dma((n - 1,)),
                dma((n - 1,)),
                pltpu.SemaphoreType.REGULAR((-(-(n - 1) // reach), 2)),
            ],
            compiler_params=pltpu.CompilerParams(
                collective_id=0, has_side_effects=True, vmem_limit_bytes=40 * 1024 * 1024
            ),
            cost_estimate=pl.CostEstimate(
                flops=14 * heads * rows * rows * size, bytes_accessed=20 * rows * width,
                transcendentals=heads * rows * rows,
            ),
            name="segment_backward",
        )(*(pltpu.with_memory_space_constraint(x, pltpu.HBM) for x in (doc_index, gate_logit, queries, key_vectors, value_vectors, out_grad)))
        return pl.pallas_call(
            functools.partial(write, heads),
            out_shape=(wide, wide, wide, jax.ShapeDtypeStruct((heads,), F32)),
            in_specs=[vmem] * 4,
            out_specs=(hbm, hbm, hbm, smem),
            scratch_shapes=[dma((3,))],
            compiler_params=pltpu.CompilerParams(vmem_limit_bytes=16 * 1024 * 1024),
            cost_estimate=pl.CostEstimate(
                flops=8 * rows * width * size, bytes_accessed=12 * rows * width,
                transcendentals=rows * width,
            ),
            name="segment_finish",
        )(*local)

    spec = P("seq", "head")
    return jax.shard_map(
        per_device, mesh=mesh, in_specs=(spec, spec, spec, spec, P("head"), P()),
        out_specs=(spec, spec, spec, P("head")), check_vma=False,
    )
```

```python
import functools
import math

import jax
import jax.numpy as jnp
from jax import lax
from jax.experimental import pallas as pl
from jax.experimental.pallas import tpu as pltpu
from jax.sharding import PartitionSpec as P

MESH = pl.DeviceIdType.MESH
F32 = jnp.float32
BF16 = jnp.bfloat16


def slope(x):
    return jnp.exp(jnp.minimum(x, 0.0))


def dot_nn(a, b):
    return lax.dot_general(a, b, (((1,), (0,)), ((), ())), preferred_element_type=F32)


def dot_nt(a, b):
    return lax.dot_general(a, b, (((1,), (1,)), ((), ())), preferred_element_type=F32)


def dot_tn(a, b):
    return lax.dot_general(a, b, (((0,), (0,)), ((), ())), preferred_element_type=F32)


def split(x):
    high = x.astype(BF16)
    return high, (x - high.astype(F32)).astype(BF16)


def merged(*lists):
    order = []
    for which, items in enumerate(lists):
        for at, item in enumerate(items):
            order.append(((at + 0.5) / len(items), which, at, item))
    return [entry[3] for entry in sorted(order, key=lambda entry: entry[:3])]


def kernel(
    n, steps, reach, heads, size, block,
    doc_hbm, logit_hbm, q_hbm, k_hbm, v_hbm, g_hbm,
    qo, ko, vo, gate_o,
    doc_ref, logit_ref, q_ref, k_ref, v_ref, g_ref, load_sem,
    kf, qf, k_slope, q_slope, extra, inv_den, s_buf, g_buf, k_turned, gate_rows, gate_all,
    norm_src, norm_got, norm_sum, mem_src, mem_got, mem_sum,
    norm_send, norm_recv, mem_send, mem_recv, gate_send, gate_recv, entered,
):
    me = lax.axis_index("seq")
    rows = q_ref.shape[0]
    blocks = rows // block
    scale = size ** -0.5
    factor = scale * math.log2(math.e)
    signs = (1, -1)
    barrier = pltpu.get_barrier_semaphore()
    loads = [
        pltpu.make_async_copy(source, target, load_sem.at[i])
        for i, (source, target) in enumerate((
            (k_hbm, k_ref), (v_hbm, v_ref), (q_hbm, q_ref), (g_hbm, g_ref),
            (doc_hbm, doc_ref), (logit_hbm, logit_ref),
        ))
    ]
    for i in (0, 4, 5, 1, 2, 3):
        loads[i].start()

    def peer(way, dist):
        return {"seq": lax.rem(me + signs[way] * dist + n, n)}

    def can_send(way, dist):
        return me + dist < n if way == 0 else me >= dist

    def can_recv(way, dist):
        return me >= dist if way == 0 else me + dist < n

    for dist in range(1, reach + 1):
        for way in range(2):
            @pl.when(can_send(way, dist))
            def _():
                pl.semaphore_signal(barrier, inc=1, device_id=peer(way, dist), device_id_type=MESH)

    def cols(h):
        return slice(h * size, (h + 1) * size)

    def part(i):
        return slice(i * block, (i + 1) * block)

    def share(h, width):
        return 1.0 / (1.0 + jnp.exp(-jnp.full((1, width), logit_ref[h], F32)))

    def weight(way, dist):
        other = lax.rem(me - signs[way] * dist + n, n)
        return jnp.where(doc_ref[other] == doc_ref[me], 1.0, 0.0).astype(F32)

    def norm_copy(way, dist):
        return pltpu.make_async_remote_copy(
            src_ref=norm_src.at[way], dst_ref=norm_got.at[way, dist - 1],
            send_sem=norm_send.at[way, dist - 1], recv_sem=norm_recv.at[way, dist - 1],
            device_id=peer(way, dist), device_id_type=MESH,
        )

    def mem_copy(way, step, h):
        return pltpu.make_async_remote_copy(
            src_ref=mem_src.at[way, step, h], dst_ref=mem_got.at[way, step, h],
            send_sem=mem_send.at[way, step, h], recv_sem=mem_recv.at[way, step, h],
            device_id=peer(way, 1 << step), device_id_type=MESH,
        )

    def gate_copy(other):
        return pltpu.make_async_remote_copy(
            src_ref=gate_rows, dst_ref=gate_all.at[me],
            send_sem=gate_send, recv_sem=gate_recv,
            device_id={"seq": lax.rem(me + other, n)}, device_id_type=MESH,
        )

    def tell(turn):
        for way in range(2):
            @pl.when(can_send(way, reach))
            def _():
                pl.semaphore_signal(entered.at[turn, way], inc=1, device_id=peer(way, reach), device_id_type=MESH)

    def hear(turn):
        for way in range(2):
            @pl.when(can_recv(way, reach))
            def _():
                pl.semaphore_wait(entered.at[turn, way], 1)

    def send_norms(way):
        for dist in range(1, reach + 1):
            @pl.when(can_send(way, dist))
            def _():
                norm_copy(way, dist).start()

    def take_norms(way):
        norm_sum[way] = jnp.zeros_like(norm_sum[way])
        for dist in range(1, reach + 1):
            @pl.when(can_recv(way, dist))
            def _():
                norm_copy(way, dist).wait_recv()
                norm_sum[way] += weight(way, dist) * norm_got[way, dist - 1]

    def send_mem(way, step, h):
        @pl.when(can_send(way, 1 << step))
        def _():
            mem_copy(way, step, h).start()

    def take_mem(way, step, h):
        if step == 0:
            mem_sum[way, h] = jnp.zeros_like(mem_sum[way, h])

        @pl.when(can_recv(way, 1 << step))
        def _():
            mem_copy(way, step, h).wait_recv()
            mem_sum[way, h] += weight(way, 1 << step) * mem_got[way, step, h]

        if step + 1 < steps:
            mem_src[way, step + 1, h] = mem_src[way, 0, h] + mem_sum[way, h]
            send_mem(way, step + 1, h)

    units = [(h, i) for h in range(heads) for i in range(blocks)]
    kept = [{} for _ in units]

    def scores(u):
        h, i = units[u]
        held = s_buf.at[u % 3]

        def tile(j):
            def run():
                if i == 0:
                    k_turned[h] = k_ref[:, cols(h)].T
                out = dot_nt(k_ref[part(j), cols(h)], q_ref[part(i), cols(h)])
                if j == i:
                    key_ids = lax.broadcasted_iota(jnp.int32, (block, block), 0)
                    query_ids = lax.broadcasted_iota(jnp.int32, (block, block), 1)
                    out = jnp.where(key_ids <= query_ids, out, -1e30)
                held[part(j), :] = out
                top = jnp.max(out, axis=0, keepdims=True)
                kept[u]["top"] = top if j == 0 else jnp.maximum(kept[u]["top"], top)
            return run

        return [tile(j) for j in range(i + 1)]

    def weights(u):
        h, i = units[u]
        held = s_buf.at[u % 3]
        grads = g_buf.at[u % 2]

        def raise_tile(j):
            def run():
                out = jnp.exp2((held[part(j), :] - kept[u]["top"]) * factor)
                held[part(j), :] = out
                total = jnp.sum(out, axis=0, keepdims=True)
                kept[u]["total"] = total if j == 0 else kept[u]["total"] + total
                if j == i:
                    kept[u]["inverse"] = 1.0 / kept[u]["total"]
            return run

        def grad_tile(j):
            def run():
                g_i = g_ref[part(i), cols(h)]
                grad = dot_nt(v_ref[part(j), cols(h)], g_i)
                grads[part(j), :] = grad
                out = held[part(j), :]
                low = (out * kept[u]["inverse"]).astype(BF16)
                delta = jnp.sum(grad * out, axis=0, keepdims=True)
                kept[u]["delta"] = delta if j == 0 else kept[u]["delta"] + delta
                piece = dot_nn(low, g_i)
                if j == i:
                    vo[part(j), cols(h)] = piece
                    kept[u]["delta"] = kept[u]["delta"] * kept[u]["inverse"]
                    kept[u]["scaled"] = kept[u]["inverse"] * (1.0 - share(h, block))
                else:
                    vo[part(j), cols(h)] += piece
            return run

        return [raise_tile(j) for j in range(i + 1)] + [grad_tile(j) for j in range(i + 1)]

    def grads(u):
        h, i = units[u]
        held = s_buf.at[u % 3]
        grads = g_buf.at[u % 2]

        def tile(j):
            def run():
                q_i = q_ref[part(i), cols(h)]
                score = held[part(j), :] * ((grads[part(j), :] - kept[u]["delta"]) * kept[u]["scaled"])
                score = score.astype(BF16)
                piece = dot_nn(score, q_i)
                if j == i:
                    ko[part(j), cols(h)] = piece
                else:
                    ko[part(j), cols(h)] += piece
                turned = dot_nn(k_turned[h, :, part(j)], score)
                kept[u]["turned"] = turned if j == 0 else kept[u]["turned"] + turned
                if j == i:
                    qo[part(i), cols(h)] = kept[u]["turned"].T * scale
            return run

        return [tile(j) for j in range(i + 1)]

    def attend(at, *more):
        lists = [items for items in more if items]
        if 0 <= at - 2 < len(units):
            lists.append(grads(at - 2))
        if 0 <= at - 1 < len(units):
            lists.append(weights(at - 1))
        if 0 <= at < len(units):
            lists.append(scores(at))
        for run in merged(*lists):
            run()

    def memory_grads(h):
        hs = cols(h)
        held = {}

        def rows_of(i):
            def run():
                norm = norm_sum[0, h:h + 1, :]
                low = qf[part(i), hs]
                den = 1.0 + jnp.sum(low.astype(F32) * norm, axis=1, keepdims=True)
                inv = jnp.broadcast_to(1.0 / den, (block, size))
                inv_den[h, part(i), :] = inv
                num = g_ref[part(i), hs].astype(F32) * inv
                both = dot_tn(low, jnp.concatenate(split(num), axis=1))
                held["both"] = both if i == 0 else held["both"] + both
                if i == blocks - 1:
                    both = held["both"]
                    mem_src[1, 0, h] = (both[:, :size] + both[:, size:]) * share(h, size)
            return run

        return [rows_of(i) for i in range(blocks)]

    def read_memory(h):
        hs = cols(h)
        held = {}

        def rows_of(i):
            def run():
                memory_share = share(h, size)
                norm = norm_sum[0, h:h + 1, :]
                beside = jnp.concatenate(split(mem_sum[0, h]), axis=1)
                low = qf[part(i), hs].astype(F32)
                g_i = g_ref[part(i), hs]
                inv = inv_den[h, part(i), :]
                weighted = inv * memory_share
                turned = dot_nt(jnp.concatenate([g_i, g_i], axis=1), beside)
                product = jnp.sum(low * turned, axis=1, keepdims=True)
                den_grad = -(weighted * inv) * product
                row = jnp.sum(den_grad * low, axis=0, keepdims=True)
                held["row"] = row if i == 0 else held["row"] + row
                extra[part(i), hs] = (turned * weighted + den_grad * norm) * q_slope[part(i), hs]
                if i == blocks - 1:
                    norm_src[1, h:h + 1, :] = held["row"]
                    both = jnp.sum(mem_sum[0, h] * mem_src[1, 0, h], axis=0, keepdims=True)
                    gate_rows[h:h + 1, :] += both * (1.0 - memory_share)
            return run

        return [rows_of(i) for i in range(blocks)]

    def local_gate(h):
        memory_share = share(h, size)
        row = jnp.zeros((1, size), F32)
        for i in range(blocks):
            row = row + jnp.sum(v_ref[part(i), cols(h)].astype(F32) * vo[part(i), cols(h)], axis=0, keepdims=True)
        gate_rows[h:h + 1, :] -= row * (memory_share * (1.0 - memory_share))

    def finish(h):
        hs = cols(h)
        local_share = 1.0 - share(h, size)
        high, rest = split(mem_sum[1, h])
        beside = jnp.concatenate([high, rest], axis=1)
        below = jnp.concatenate([high, rest], axis=0)
        for i in range(blocks):
            v_i = v_ref[part(i), hs]
            low = kf[part(i), hs]
            turned = dot_nt(jnp.concatenate([v_i, v_i], axis=1), beside)
            ko[part(i), hs] = ko[part(i), hs] * scale + turned * k_slope[part(i), hs]
            value = dot_nn(jnp.concatenate([low, low], axis=1), below)
            vo[part(i), hs] = vo[part(i), hs] * local_share + value
            qo[part(i), hs] += extra[part(i), hs]

    def key_memory(h):
        def run():
            mem_src[0, 0, h] = dot_tn(kf[:, cols(h)], v_ref[:, cols(h)])
        return [run]

    def query_features(h):
        def rows_of(i):
            def run():
                x = q_ref[part(i), cols(h)].astype(F32)
                flat = slope(x)
                q_slope[part(i), cols(h)] = flat
                qf[part(i), cols(h)] = (jnp.maximum(x, 0.0) + flat).astype(BF16)
            return run

        return [rows_of(i) for i in range(blocks)]

    gate_rows[...] = jnp.zeros_like(gate_rows)
    norm_src[...] = jnp.zeros_like(norm_src)
    loads[0].wait()
    for h in range(heads):
        norm = jnp.zeros((1, size), F32)
        for i in range(blocks):
            x = k_ref[part(i), cols(h)].astype(F32)
            flat = slope(x)
            k_slope[part(i), cols(h)] = flat
            low = (jnp.maximum(x, 0.0) + flat).astype(BF16)
            kf[part(i), cols(h)] = low
            norm = norm + jnp.sum(low.astype(F32), axis=0, keepdims=True)
        norm_src[0, h:h + 1, :] = norm
    for i in (4, 5, 1, 2, 3):
        loads[i].wait()
    attend(-1, *(key_memory(h) for h in range(heads)), *(query_features(h) for h in range(heads)))
    pl.semaphore_wait(barrier, jnp.minimum(me, reach) + jnp.minimum(n - 1 - me, reach))
    send_norms(0)
    for h in range(heads):
        send_mem(0, 0, h)
    turns = -(-(n - 1) // reach) - 1
    if turns:
        tell(0)

    last = len(units) + 1
    polls, reads = {}, {}
    plan = []
    if steps > 1:
        firsts = [(3, 0, 0), (4, 0, 1), (6, 0, 2), (7, 1, 0), (8, 1, 1), (9, 1, 2)]
        plan += [(at, way, 0, h) for at, way, h in firsts if h < heads]
        plan += [(last - 2, way, 0, h) for h in range(3, heads) for way in range(2)]
    if steps == 2:
        plan += [(9 + h, 0, 1, h) for h in range(min(heads, 3))]
    for at, way, step, h in plan:
        polls.setdefault(min(at, last - 1), []).append((way, step, h))
        if way == 0 and step == steps - 1:
            reads.setdefault(min(at, last - 1) + 1, []).append(h)
    taken = [h for at in reads for h in reads[at]]
    for at in range(last + 1):
        grads_now = [memory_grads(h) for h in range(heads)] if at == 3 else []
        if at == 3:
            take_norms(0)
        attend(at, *grads_now, *(read_memory(h) for h in reads.get(at, [])))
        if at == 3:
            for h in range(heads):
                send_mem(1, 0, h)
        for way, step, h in polls.get(at, []):
            take_mem(way, step, h)
        for turn in range(turns - 1):
            if at == min(5 + 2 * turn, last):
                hear(turn)
                tell(turn + 1)
    for step in range(1, steps - 1):
        for h in range(heads):
            for way in range(2):
                take_mem(way, step, h)
    for h in range(heads):
        if h not in taken:
            take_mem(0, steps - 1, h)
            attend(-1, read_memory(h))
    send_norms(1)
    for h in range(heads):
        local_gate(h)
    if turns:
        hear(turns - 1)
    for other in range(1, n):
        gate_copy(other).start()
    gate_all[me] = gate_rows[...]
    for h in range(heads):
        take_mem(1, steps - 1, h)
        finish(h)
    for way in range(2):
        for dist in range(1, reach + 1):
            @pl.when(can_send(way, dist))
            def _():
                norm_copy(way, dist).wait_send()
        for step in range(steps):
            @pl.when(can_send(way, 1 << step))
            def _():
                for h in range(heads):
                    mem_copy(way, step, h).wait_send()
    take_norms(1)
    for h in range(heads):
        norm = norm_sum[1, h:h + 1, :]
        for i in range(blocks):
            ko[part(i), cols(h)] += norm * k_slope[part(i), cols(h)]
    others = gate_all.at[pl.ds(0, n - 1)]
    pltpu.make_async_copy(others, others, gate_recv).wait()
    gates = gate_all[0]
    for other in range(1, n):
        gates = gates + gate_all[other]
    gate_o[...] = gates
    pltpu.make_async_copy(others, others, gate_send).wait()


def write(heads, q_ref, k_ref, v_ref, gate_ref, q_hbm, k_hbm, v_hbm, gate_o, sems):
    copies = [
        pltpu.make_async_copy(source, target, sems.at[i])
        for i, (source, target) in enumerate(((q_ref, q_hbm), (k_ref, k_hbm), (v_ref, v_hbm)))
    ]
    for copy in copies:
        copy.start()
    for h in range(heads):
        gate_o[h] = jnp.sum(gate_ref[h:h + 1, :])
    for copy in copies:
        copy.wait()


def solution(mesh):
    n = mesh.shape["seq"]
    longest = max(n // 2, 2)
    steps = (longest - 1).bit_length()
    reach = longest - 1

    def per_device(queries, key_vectors, value_vectors, out_grad, gate_logit, doc_index):
        rows, width = queries.shape
        heads = gate_logit.shape[0]
        size = width // heads
        block = min(256, rows)
        wide = jax.ShapeDtypeStruct((rows, width), F32)
        vmem = pl.BlockSpec(memory_space=pltpu.VMEM)
        smem = pl.BlockSpec(memory_space=pltpu.SMEM)
        hbm = pl.BlockSpec(memory_space=pltpu.HBM)
        tall = -(-heads // 8) * 8
        dma = pltpu.SemaphoreType.DMA
        local = pl.pallas_call(
            functools.partial(kernel, n, steps, reach, heads, size, block),
            out_shape=(wide, wide, wide, jax.ShapeDtypeStruct((tall, size), F32)),
            in_specs=[hbm] * 6,
            out_specs=(vmem,) * 4,
            scratch_shapes=[
                pltpu.SMEM(doc_index.shape, jnp.int32),
                pltpu.SMEM(gate_logit.shape, F32),
                pltpu.VMEM((rows, width), BF16),
                pltpu.VMEM((rows, width), BF16),
                pltpu.VMEM((rows, width), BF16),
                pltpu.VMEM((rows, width), BF16),
                dma((6,)),
                pltpu.VMEM((rows, width), BF16),
                pltpu.VMEM((rows, width), BF16),
                pltpu.VMEM((rows, width), F32),
                pltpu.VMEM((rows, width), F32),
                pltpu.VMEM((rows, width), F32),
                pltpu.VMEM((heads, rows, size), F32),
                pltpu.VMEM((3, rows, block), F32),
                pltpu.VMEM((2, rows, block), F32),
                pltpu.VMEM((heads, size, rows), BF16),
                pltpu.VMEM((tall, size), F32),
                pltpu.VMEM((n, tall, size), F32),
                pltpu.VMEM((2, tall, size), F32),
                pltpu.VMEM((2, reach, tall, size), F32),
                pltpu.VMEM((2, tall, size), F32),
                pltpu.VMEM((2, steps, heads, size, size), F32),
                pltpu.VMEM((2, steps, heads, size, size), F32),
                pltpu.VMEM((2, heads, size, size), F32),
                dma((2, reach)),
                dma((2, reach)),
                dma((2, steps, heads)),
                dma((2, steps, heads)),
                dma(()),
                dma(()),
                pltpu.SemaphoreType.REGULAR((-(-(n - 1) // reach), 2)),
            ],
            compiler_params=pltpu.CompilerParams(
                collective_id=0, has_side_effects=True, vmem_limit_bytes=40 * 1024 * 1024
            ),
            cost_estimate=pl.CostEstimate(
                flops=14 * heads * rows * rows * size, bytes_accessed=20 * rows * width,
                transcendentals=heads * rows * rows,
            ),
            name="segment_backward",
        )(*(pltpu.with_memory_space_constraint(x, pltpu.HBM) for x in (doc_index, gate_logit, queries, key_vectors, value_vectors, out_grad)))
        return pl.pallas_call(
            functools.partial(write, heads),
            out_shape=(wide, wide, wide, jax.ShapeDtypeStruct((heads,), F32)),
            in_specs=[vmem] * 4,
            out_specs=(hbm, hbm, hbm, smem),
            scratch_shapes=[dma((3,))],
            compiler_params=pltpu.CompilerParams(vmem_limit_bytes=16 * 1024 * 1024),
            cost_estimate=pl.CostEstimate(
                flops=8 * rows * width * size, bytes_accessed=12 * rows * width,
                transcendentals=rows * width,
            ),
            name="segment_finish",
        )(*local)

    spec = P("seq", "head")
    return jax.shard_map(
        per_device, mesh=mesh, in_specs=(spec, spec, spec, spec, P("head"), P()),
        out_specs=(spec, spec, spec, P("head")), check_vma=False,
    )
```

```python
import functools
import math

import jax
import jax.numpy as jnp
from jax import lax
from jax.experimental import pallas as pl
from jax.experimental.pallas import tpu as pltpu
from jax.sharding import PartitionSpec as P

MESH = pl.DeviceIdType.MESH
F32 = jnp.float32
BF16 = jnp.bfloat16


def slope(x):
    return jnp.exp(jnp.minimum(x, 0.0))


def dot_nn(a, b):
    return lax.dot_general(a, b, (((1,), (0,)), ((), ())), preferred_element_type=F32)


def dot_nt(a, b):
    return lax.dot_general(a, b, (((1,), (1,)), ((), ())), preferred_element_type=F32)


def dot_tn(a, b):
    return lax.dot_general(a, b, (((0,), (0,)), ((), ())), preferred_element_type=F32)


def split(x):
    high = x.astype(BF16)
    return high, (x - high.astype(F32)).astype(BF16)


def merged(*lists):
    order = []
    for which, items in enumerate(lists):
        for at, item in enumerate(items):
            order.append(((at + 0.5) / len(items), which, at, item))
    return [entry[3] for entry in sorted(order, key=lambda entry: entry[:3])]


def kernel(
    n, steps, reach, heads, size, block,
    doc_hbm, logit_hbm, q_hbm, k_hbm, v_hbm, g_hbm,
    qo, ko, vo, gate_o,
    doc_ref, logit_ref, q_ref, k_ref, v_ref, g_ref, load_sem,
    kf, qf, k_slope, q_slope, extra, inv_den, s_buf, g_buf, k_turned, gate_rows, gate_all,
    norm_src, norm_got, norm_sum, mem_src, mem_got, mem_sum,
    norm_send, norm_recv, mem_send, mem_recv, gate_send, gate_recv, entered,
):
    me = lax.axis_index("seq")
    rows = q_ref.shape[0]
    blocks = rows // block
    scale = size ** -0.5
    factor = scale * math.log2(math.e)
    signs = (1, -1)
    barrier = pltpu.get_barrier_semaphore()
    loads = [
        pltpu.make_async_copy(source, target, load_sem.at[i])
        for i, (source, target) in enumerate((
            (k_hbm, k_ref), (v_hbm, v_ref), (q_hbm, q_ref), (g_hbm, g_ref),
            (doc_hbm, doc_ref), (logit_hbm, logit_ref),
        ))
    ]
    for i in (0, 4, 5, 1, 2, 3):
        loads[i].start()

    def peer(way, dist):
        return {"seq": lax.rem(me + signs[way] * dist + n, n)}

    def can_send(way, dist):
        return me + dist < n if way == 0 else me >= dist

    def can_recv(way, dist):
        return me >= dist if way == 0 else me + dist < n

    for dist in range(1, reach + 1):
        for way in range(2):
            @pl.when(can_send(way, dist))
            def _():
                pl.semaphore_signal(barrier, inc=1, device_id=peer(way, dist), device_id_type=MESH)

    def cols(h):
        return slice(h * size, (h + 1) * size)

    def part(i):
        return slice(i * block, (i + 1) * block)

    def share(h, width):
        return 1.0 / (1.0 + jnp.exp(-jnp.full((1, width), logit_ref[h], F32)))

    def weight(way, dist):
        other = lax.rem(me - signs[way] * dist + n, n)
        return jnp.where(doc_ref[other] == doc_ref[me], 1.0, 0.0).astype(F32)

    def norm_copy(way, dist):
        return pltpu.make_async_remote_copy(
            src_ref=norm_src.at[way], dst_ref=norm_got.at[way, dist - 1],
            send_sem=norm_send.at[way, dist - 1], recv_sem=norm_recv.at[way, dist - 1],
            device_id=peer(way, dist), device_id_type=MESH,
        )

    def mem_copy(way, step, h):
        return pltpu.make_async_remote_copy(
            src_ref=mem_src.at[way, step, h], dst_ref=mem_got.at[way, step, h],
            send_sem=mem_send.at[way, step], recv_sem=mem_recv.at[way, step, h],
            device_id=peer(way, 1 << step), device_id_type=MESH,
        )

    def gate_copy(other):
        return pltpu.make_async_remote_copy(
            src_ref=gate_rows, dst_ref=gate_all.at[me],
            send_sem=gate_send, recv_sem=gate_recv,
            device_id={"seq": lax.rem(me + other, n)}, device_id_type=MESH,
        )

    def tell(turn):
        for way in range(2):
            @pl.when(can_send(way, reach))
            def _():
                pl.semaphore_signal(entered.at[turn, way], inc=1, device_id=peer(way, reach), device_id_type=MESH)

    def hear(turn):
        for way in range(2):
            @pl.when(can_recv(way, reach))
            def _():
                pl.semaphore_wait(entered.at[turn, way], 1)

    def send_norms(way):
        for dist in range(1, reach + 1):
            @pl.when(can_send(way, dist))
            def _():
                norm_copy(way, dist).start()

    def take_norms(way):
        norm_sum[way] = jnp.zeros_like(norm_sum[way])
        for dist in range(1, reach + 1):
            @pl.when(can_recv(way, dist))
            def _():
                norm_copy(way, dist).wait_recv()
                norm_sum[way] += weight(way, dist) * norm_got[way, dist - 1]

    def send_mem(way, step, h):
        @pl.when(can_send(way, 1 << step))
        def _():
            mem_copy(way, step, h).start()

    def take_mem(way, step, h):
        if step == 0:
            mem_sum[way, h] = jnp.zeros_like(mem_sum[way, h])

        @pl.when(can_recv(way, 1 << step))
        def _():
            mem_copy(way, step, h).wait_recv()
            mem_sum[way, h] += weight(way, 1 << step) * mem_got[way, step, h]

        if step + 1 < steps:
            mem_src[way, step + 1, h] = mem_src[way, 0, h] + mem_sum[way, h]
            send_mem(way, step + 1, h)

    units = [(h, i) for h in range(heads) for i in range(blocks)]
    kept = [{} for _ in units]

    def scores(u):
        h, i = units[u]
        held = s_buf.at[u % 3]

        def tile(j):
            def run():
                if i == 0:
                    k_turned[h] = k_ref[:, cols(h)].T
                out = dot_nt(k_ref[part(j), cols(h)], q_ref[part(i), cols(h)])
                if j == i:
                    key_ids = lax.broadcasted_iota(jnp.int32, (block, block), 0)
                    query_ids = lax.broadcasted_iota(jnp.int32, (block, block), 1)
                    out = jnp.where(key_ids <= query_ids, out, -1e30)
                held[part(j), :] = out
                top = jnp.max(out, axis=0, keepdims=True)
                kept[u]["top"] = top if j == 0 else jnp.maximum(kept[u]["top"], top)
            return run

        return [tile(j) for j in range(i + 1)]

    def weights(u):
        h, i = units[u]
        held = s_buf.at[u % 3]
        grads = g_buf.at[u % 2]

        def raise_tile(j):
            def run():
                out = jnp.exp2((held[part(j), :] - kept[u]["top"]) * factor)
                held[part(j), :] = out
                total = jnp.sum(out, axis=0, keepdims=True)
                kept[u]["total"] = total if j == 0 else kept[u]["total"] + total
                if j == i:
                    kept[u]["inverse"] = 1.0 / kept[u]["total"]
            return run

        def grad_tile(j):
            def run():
                g_i = g_ref[part(i), cols(h)]
                grad = dot_nt(v_ref[part(j), cols(h)], g_i)
                grads[part(j), :] = grad
                out = held[part(j), :]
                low = (out * kept[u]["inverse"]).astype(BF16)
                delta = jnp.sum(grad * out, axis=0, keepdims=True)
                kept[u]["delta"] = delta if j == 0 else kept[u]["delta"] + delta
                piece = dot_nn(low, g_i)
                if j == i:
                    vo[part(j), cols(h)] = piece
                    kept[u]["delta"] = kept[u]["delta"] * kept[u]["inverse"]
                    kept[u]["scaled"] = kept[u]["inverse"] * (1.0 - share(h, block))
                else:
                    vo[part(j), cols(h)] += piece
            return run

        return [raise_tile(j) for j in range(i + 1)] + [grad_tile(j) for j in range(i + 1)]

    def grads(u):
        h, i = units[u]
        held = s_buf.at[u % 3]
        grads = g_buf.at[u % 2]

        def tile(j):
            def run():
                q_i = q_ref[part(i), cols(h)]
                score = held[part(j), :] * ((grads[part(j), :] - kept[u]["delta"]) * kept[u]["scaled"])
                score = score.astype(BF16)
                piece = dot_nn(score, q_i)
                if j == i:
                    ko[part(j), cols(h)] = piece
                else:
                    ko[part(j), cols(h)] += piece
                turned = dot_nn(k_turned[h, :, part(j)], score)
                kept[u]["turned"] = turned if j == 0 else kept[u]["turned"] + turned
                if j == i:
                    qo[part(i), cols(h)] = kept[u]["turned"].T * scale
            return run

        return [tile(j) for j in range(i + 1)]

    def attend(at, *more):
        lists = [items for items in more if items]
        if 0 <= at - 2 < len(units):
            lists.append(grads(at - 2))
        if 0 <= at - 1 < len(units):
            lists.append(weights(at - 1))
        if 0 <= at < len(units):
            lists.append(scores(at))
        for run in merged(*lists):
            run()

    def memory_grads(h):
        hs = cols(h)
        held = {}

        def rows_of(i):
            def run():
                norm = norm_sum[0, h:h + 1, :]
                low = qf[part(i), hs]
                den = 1.0 + jnp.sum(low.astype(F32) * norm, axis=1, keepdims=True)
                inv = jnp.broadcast_to(1.0 / den, (block, size))
                inv_den[h, part(i), :] = inv
                num = g_ref[part(i), hs].astype(F32) * inv
                both = dot_tn(low, jnp.concatenate(split(num), axis=1))
                held["both"] = both if i == 0 else held["both"] + both
                if i == blocks - 1:
                    both = held["both"]
                    mem_src[1, 0, h] = (both[:, :size] + both[:, size:]) * share(h, size)
            return run

        return [rows_of(i) for i in range(blocks)]

    def read_memory(h):
        hs = cols(h)
        held = {}

        def rows_of(i):
            def run():
                memory_share = share(h, size)
                norm = norm_sum[0, h:h + 1, :]
                beside = jnp.concatenate(split(mem_sum[0, h]), axis=1)
                low = qf[part(i), hs].astype(F32)
                g_i = g_ref[part(i), hs]
                inv = inv_den[h, part(i), :]
                weighted = inv * memory_share
                turned = dot_nt(jnp.concatenate([g_i, g_i], axis=1), beside)
                product = jnp.sum(low * turned, axis=1, keepdims=True)
                den_grad = -(weighted * inv) * product
                row = jnp.sum(den_grad * low, axis=0, keepdims=True)
                held["row"] = row if i == 0 else held["row"] + row
                extra[part(i), hs] = (turned * weighted + den_grad * norm) * q_slope[part(i), hs]
                if i == blocks - 1:
                    norm_src[1, h:h + 1, :] = held["row"]
                    both = jnp.sum(mem_sum[0, h] * mem_src[1, 0, h], axis=0, keepdims=True)
                    gate_rows[h:h + 1, :] += both * (1.0 - memory_share)
            return run

        return [rows_of(i) for i in range(blocks)]

    def local_gate(h):
        held = {}

        def rows_of(i):
            def run():
                product = v_ref[part(i), cols(h)].astype(F32) * vo[part(i), cols(h)]
                row = jnp.sum(product, axis=0, keepdims=True)
                held["row"] = row if i == 0 else held["row"] + row
                if i == blocks - 1:
                    memory_share = share(h, size)
                    gate_rows[h:h + 1, :] -= held["row"] * (memory_share * (1.0 - memory_share))
            return run

        return [rows_of(i) for i in range(blocks)]

    def finish(h):
        hs = cols(h)
        local_share = 1.0 - share(h, size)
        high, rest = split(mem_sum[1, h])
        beside = jnp.concatenate([high, rest], axis=1)
        below = jnp.concatenate([high, rest], axis=0)
        for i in range(blocks):
            v_i = v_ref[part(i), hs]
            low = kf[part(i), hs]
            turned = dot_nt(jnp.concatenate([v_i, v_i], axis=1), beside)
            ko[part(i), hs] = ko[part(i), hs] * scale + turned * k_slope[part(i), hs]
            value = dot_nn(jnp.concatenate([low, low], axis=1), below)
            vo[part(i), hs] = vo[part(i), hs] * local_share + value
            qo[part(i), hs] += extra[part(i), hs]

    def key_memory(h):
        def run():
            mem_src[0, 0, h] = dot_tn(kf[:, cols(h)], v_ref[:, cols(h)])
        return [run]

    def query_features(h):
        def rows_of(i):
            def run():
                x = q_ref[part(i), cols(h)].astype(F32)
                flat = slope(x)
                q_slope[part(i), cols(h)] = flat
                qf[part(i), cols(h)] = (jnp.maximum(x, 0.0) + flat).astype(BF16)
            return run

        return [rows_of(i) for i in range(blocks)]

    gate_rows[...] = jnp.zeros_like(gate_rows)
    norm_src[...] = jnp.zeros_like(norm_src)
    loads[0].wait()
    for h in range(heads):
        norm = jnp.zeros((1, size), F32)
        for i in range(blocks):
            x = k_ref[part(i), cols(h)].astype(F32)
            flat = slope(x)
            k_slope[part(i), cols(h)] = flat
            low = (jnp.maximum(x, 0.0) + flat).astype(BF16)
            kf[part(i), cols(h)] = low
            norm = norm + jnp.sum(low.astype(F32), axis=0, keepdims=True)
        norm_src[0, h:h + 1, :] = norm
    for i in (4, 5, 1, 2, 3):
        loads[i].wait()
    attend(-1, *(key_memory(h) for h in range(heads)), *(query_features(h) for h in range(heads)))
    pl.semaphore_wait(barrier, jnp.minimum(me, reach) + jnp.minimum(n - 1 - me, reach))
    send_norms(0)
    for h in range(heads):
        send_mem(0, 0, h)
    turns = -(-(n - 1) // reach) - 1
    if turns:
        tell(0)

    last = len(units) + 1
    polls, reads = {}, {}
    plan = []
    if steps > 1:
        firsts = [(5, 0, 0), (7, 0, 1), (9, 0, 2), (10, 1, 0), (11, 1, 1), (12, 1, 2)]
        plan += [(at, way, 0, h) for at, way, h in firsts if h < heads]
        plan += [(last - 2, way, 0, h) for h in range(3, heads) for way in range(2)]
    if steps == 2:
        plan = [(10 + h, 0, 1, h) for h in range(min(heads, 3))] + plan
    for at, way, step, h in plan:
        polls.setdefault(min(at, last - 1), []).append((way, step, h))
        if way == 0 and step == steps - 1:
            reads.setdefault(min(at, last - 1) + 1, []).append(h)
    taken = [h for at in reads for h in reads[at]]
    begin = min(5, last - 1)
    for at in range(last + 1):
        grads_now = [memory_grads(at - begin)] if begin < at < begin + heads else []
        parts = grads_now + [read_memory(h) for h in reads.get(at, [])]
        parts += [local_gate(h) for h in range(heads) if at == (h + 1) * blocks + 1]
        attend(at, *parts)
        if grads_now:
            send_mem(1, 0, at - begin)
        if at == begin:
            take_norms(0)
            attend(-1, memory_grads(0))
            send_mem(1, 0, 0)
        for way, step, h in polls.get(at, []):
            take_mem(way, step, h)
        for turn in range(turns - 1):
            if at == min(6 + 2 * turn, last):
                hear(turn)
                tell(turn + 1)
    for h in range(last - begin + 1, heads):
        attend(-1, memory_grads(h))
        send_mem(1, 0, h)
    for step in range(1, steps - 1):
        for h in range(heads):
            for way in range(2):
                take_mem(way, step, h)
    for h in range(heads):
        if h not in taken:
            take_mem(0, steps - 1, h)
            attend(-1, read_memory(h))
    send_norms(1)
    if turns:
        hear(turns - 1)
    for other in range(1, n):
        gate_copy(other).start()
    gate_all[me] = gate_rows[...]
    for h in range(heads):
        take_mem(1, steps - 1, h)
        finish(h)
    for way in range(2):
        for dist in range(1, reach + 1):
            @pl.when(can_send(way, dist))
            def _():
                norm_copy(way, dist).wait_send()
        for step in range(steps):
            @pl.when(can_send(way, 1 << step))
            def _():
                pltpu.make_async_copy(mem_src.at[way, step], mem_src.at[way, step], mem_send.at[way, step]).wait()
    take_norms(1)
    for h in range(heads):
        norm = norm_sum[1, h:h + 1, :]
        for i in range(blocks):
            ko[part(i), cols(h)] += norm * k_slope[part(i), cols(h)]
    others = gate_all.at[pl.ds(0, n - 1)]
    pltpu.make_async_copy(others, others, gate_recv).wait()
    gates = gate_all[0]
    for other in range(1, n):
        gates = gates + gate_all[other]
    gate_o[...] = gates
    pltpu.make_async_copy(others, others, gate_send).wait()


def write(heads, q_ref, k_ref, v_ref, gate_ref, q_hbm, k_hbm, v_hbm, gate_o, sems):
    copies = [
        pltpu.make_async_copy(source, target, sems.at[i])
        for i, (source, target) in enumerate(((q_ref, q_hbm), (k_ref, k_hbm), (v_ref, v_hbm)))
    ]
    for copy in copies:
        copy.start()
    for h in range(heads):
        gate_o[h] = jnp.sum(gate_ref[h:h + 1, :])
    for copy in copies:
        copy.wait()


def solution(mesh):
    n = mesh.shape["seq"]
    longest = max(n // 2, 2)
    steps = (longest - 1).bit_length()
    reach = longest - 1

    def per_device(queries, key_vectors, value_vectors, out_grad, gate_logit, doc_index):
        rows, width = queries.shape
        heads = gate_logit.shape[0]
        size = width // heads
        block = min(256, rows)
        wide = jax.ShapeDtypeStruct((rows, width), F32)
        vmem = pl.BlockSpec(memory_space=pltpu.VMEM)
        smem = pl.BlockSpec(memory_space=pltpu.SMEM)
        hbm = pl.BlockSpec(memory_space=pltpu.HBM)
        tall = -(-heads // 8) * 8
        dma = pltpu.SemaphoreType.DMA
        local = pl.pallas_call(
            functools.partial(kernel, n, steps, reach, heads, size, block),
            out_shape=(wide, wide, wide, jax.ShapeDtypeStruct((tall, size), F32)),
            in_specs=[hbm] * 6,
            out_specs=(vmem,) * 4,
            scratch_shapes=[
                pltpu.SMEM(doc_index.shape, jnp.int32),
                pltpu.SMEM(gate_logit.shape, F32),
                pltpu.VMEM((rows, width), BF16),
                pltpu.VMEM((rows, width), BF16),
                pltpu.VMEM((rows, width), BF16),
                pltpu.VMEM((rows, width), BF16),
                dma((6,)),
                pltpu.VMEM((rows, width), BF16),
                pltpu.VMEM((rows, width), BF16),
                pltpu.VMEM((rows, width), F32),
                pltpu.VMEM((rows, width), F32),
                pltpu.VMEM((rows, width), F32),
                pltpu.VMEM((heads, rows, size), F32),
                pltpu.VMEM((3, rows, block), F32),
                pltpu.VMEM((2, rows, block), F32),
                pltpu.VMEM((heads, size, rows), BF16),
                pltpu.VMEM((tall, size), F32),
                pltpu.VMEM((n, tall, size), F32),
                pltpu.VMEM((2, tall, size), F32),
                pltpu.VMEM((2, reach, tall, size), F32),
                pltpu.VMEM((2, tall, size), F32),
                pltpu.VMEM((2, steps, heads, size, size), F32),
                pltpu.VMEM((2, steps, heads, size, size), F32),
                pltpu.VMEM((2, heads, size, size), F32),
                dma((2, reach)),
                dma((2, reach)),
                dma((2, steps)),
                dma((2, steps, heads)),
                dma(()),
                dma(()),
                pltpu.SemaphoreType.REGULAR((max(-(-(n - 1) // reach) - 1, 1), 2)),
            ],
            compiler_params=pltpu.CompilerParams(
                collective_id=0, has_side_effects=True, vmem_limit_bytes=40 * 1024 * 1024
            ),
            cost_estimate=pl.CostEstimate(
                flops=14 * heads * rows * rows * size, bytes_accessed=20 * rows * width,
                transcendentals=heads * rows * rows,
            ),
            name="segment_backward",
        )(*(pltpu.with_memory_space_constraint(x, pltpu.HBM) for x in (doc_index, gate_logit, queries, key_vectors, value_vectors, out_grad)))
        return pl.pallas_call(
            functools.partial(write, heads),
            out_shape=(wide, wide, wide, jax.ShapeDtypeStruct((heads,), F32)),
            in_specs=[vmem] * 4,
            out_specs=(hbm, hbm, hbm, smem),
            scratch_shapes=[dma((3,))],
            compiler_params=pltpu.CompilerParams(vmem_limit_bytes=16 * 1024 * 1024),
            cost_estimate=pl.CostEstimate(
                flops=8 * rows * width * size, bytes_accessed=12 * rows * width,
                transcendentals=rows * width,
            ),
            name="segment_finish",
        )(*local)

    spec = P("seq", "head")
    return jax.shard_map(
        per_device, mesh=mesh, in_specs=(spec, spec, spec, spec, P("head"), P()),
        out_specs=(spec, spec, spec, P("head")), check_vma=False,
    )
```

```python
import functools
import math

import jax
import jax.numpy as jnp
from jax import lax
from jax.experimental import pallas as pl
from jax.experimental.pallas import tpu as pltpu
from jax.sharding import PartitionSpec as P

MESH = pl.DeviceIdType.MESH
F32 = jnp.float32
BF16 = jnp.bfloat16


def slope(x):
    return jnp.exp(jnp.minimum(x, 0.0))


def dot_nn(a, b):
    return lax.dot_general(a, b, (((1,), (0,)), ((), ())), preferred_element_type=F32)


def dot_nt(a, b):
    return lax.dot_general(a, b, (((1,), (1,)), ((), ())), preferred_element_type=F32)


def dot_tn(a, b):
    return lax.dot_general(a, b, (((0,), (0,)), ((), ())), preferred_element_type=F32)


def split(x):
    high = x.astype(BF16)
    return high, (x - high.astype(F32)).astype(BF16)


def merged(*lists):
    order = []
    for which, items in enumerate(lists):
        for at, item in enumerate(items):
            order.append(((at + 0.5) / len(items), which, at, item))
    return [entry[3] for entry in sorted(order, key=lambda entry: entry[:3])]


def kernel(
    n, steps, reach, heads, size, block,
    doc_hbm, logit_hbm, q_hbm, k_hbm, v_hbm, g_hbm,
    qo, ko, vo, gate_o,
    doc_ref, logit_ref, q_ref, k_ref, v_ref, g_ref, load_sem,
    kf, qf, k_slope, q_slope, extra, inv_den, s_buf, g_buf, k_turned, gate_rows, gate_all,
    norm_src, norm_got, norm_sum, mem_src, mem_got, mem_sum,
    norm_send, norm_recv, mem_send, mem_recv, gate_send, gate_recv, entered,
):
    me = lax.axis_index("seq")
    rows = q_ref.shape[0]
    blocks = rows // block
    scale = size ** -0.5
    factor = scale * math.log2(math.e)
    signs = (1, -1)
    barrier = pltpu.get_barrier_semaphore()
    loads = [
        pltpu.make_async_copy(source, target, load_sem.at[i])
        for i, (source, target) in enumerate((
            (k_hbm, k_ref), (v_hbm, v_ref), (q_hbm, q_ref), (g_hbm, g_ref),
            (doc_hbm, doc_ref), (logit_hbm, logit_ref),
        ))
    ]
    for i in (0, 4, 5, 1, 2, 3):
        loads[i].start()

    def peer(way, dist):
        return {"seq": lax.rem(me + signs[way] * dist + n, n)}

    def can_send(way, dist):
        return me + dist < n if way == 0 else me >= dist

    def can_recv(way, dist):
        return me >= dist if way == 0 else me + dist < n

    for dist in range(1, reach + 1):
        for way in range(2):
            @pl.when(can_send(way, dist))
            def _():
                pl.semaphore_signal(barrier, inc=1, device_id=peer(way, dist), device_id_type=MESH)

    def cols(h):
        return slice(h * size, (h + 1) * size)

    def part(i):
        return slice(i * block, (i + 1) * block)

    def share(h, width):
        return 1.0 / (1.0 + jnp.exp(-jnp.full((1, width), logit_ref[h], F32)))

    def weight(way, dist):
        other = lax.rem(me - signs[way] * dist + n, n)
        return jnp.where(doc_ref[other] == doc_ref[me], 1.0, 0.0).astype(F32)

    def norm_copy(way, dist):
        return pltpu.make_async_remote_copy(
            src_ref=norm_src.at[way], dst_ref=norm_got.at[way, dist - 1],
            send_sem=norm_send.at[way, dist - 1], recv_sem=norm_recv.at[way, dist - 1],
            device_id=peer(way, dist), device_id_type=MESH,
        )

    def mem_copy(way, step, h):
        return pltpu.make_async_remote_copy(
            src_ref=mem_src.at[way, step, h], dst_ref=mem_got.at[way, step, h],
            send_sem=mem_send.at[way, step], recv_sem=mem_recv.at[way, step, h],
            device_id=peer(way, 1 << step), device_id_type=MESH,
        )

    def gate_copy(other):
        return pltpu.make_async_remote_copy(
            src_ref=gate_rows, dst_ref=gate_all.at[me],
            send_sem=gate_send, recv_sem=gate_recv,
            device_id={"seq": lax.rem(me + other, n)}, device_id_type=MESH,
        )

    def tell(turn):
        for way in range(2):
            @pl.when(can_send(way, reach))
            def _():
                pl.semaphore_signal(entered.at[turn, way], inc=1, device_id=peer(way, reach), device_id_type=MESH)

    def hear(turn):
        for way in range(2):
            @pl.when(can_recv(way, reach))
            def _():
                pl.semaphore_wait(entered.at[turn, way], 1)

    def send_norms(way):
        for dist in range(1, reach + 1):
            @pl.when(can_send(way, dist))
            def _():
                norm_copy(way, dist).start()

    def take_norms(way):
        norm_sum[way] = jnp.zeros_like(norm_sum[way])
        for dist in range(1, reach + 1):
            @pl.when(can_recv(way, dist))
            def _():
                norm_copy(way, dist).wait_recv()
                norm_sum[way] += weight(way, dist) * norm_got[way, dist - 1]

    def send_mem(way, step, h):
        @pl.when(can_send(way, 1 << step))
        def _():
            mem_copy(way, step, h).start()

    def take_mem(way, step, h):
        if step == 0:
            mem_sum[way, h] = jnp.zeros_like(mem_sum[way, h])

        @pl.when(can_recv(way, 1 << step))
        def _():
            mem_copy(way, step, h).wait_recv()
            mem_sum[way, h] += weight(way, 1 << step) * mem_got[way, step, h]

        if step + 1 < steps:
            mem_src[way, step + 1, h] = mem_src[way, 0, h] + mem_sum[way, h]
            send_mem(way, step + 1, h)

    units = [(h, i) for h in range(heads) for i in range(blocks)]
    kept = [{} for _ in units]

    def scores(u):
        h, i = units[u]
        held = s_buf.at[u % 3]

        def tile(j):
            def run():
                if i == 0:
                    k_turned[h] = k_ref[:, cols(h)].T
                out = dot_nt(k_ref[part(j), cols(h)], q_ref[part(i), cols(h)])
                if j == i:
                    key_ids = lax.broadcasted_iota(jnp.int32, (block, block), 0)
                    query_ids = lax.broadcasted_iota(jnp.int32, (block, block), 1)
                    out = jnp.where(key_ids <= query_ids, out, -1e30)
                held[part(j), :] = out
                top = jnp.max(out, axis=0, keepdims=True)
                kept[u]["top"] = top if j == 0 else jnp.maximum(kept[u]["top"], top)
            return run

        return [tile(j) for j in range(i + 1)]

    def weights(u):
        h, i = units[u]
        held = s_buf.at[u % 3]
        grads = g_buf.at[u % 2]

        def raise_tile(j):
            def run():
                out = jnp.exp2((held[part(j), :] - kept[u]["top"]) * factor)
                held[part(j), :] = out
                total = jnp.sum(out, axis=0, keepdims=True)
                kept[u]["total"] = total if j == 0 else kept[u]["total"] + total
                if j == i:
                    kept[u]["inverse"] = 1.0 / kept[u]["total"]
            return run

        def grad_tile(j):
            def run():
                g_i = g_ref[part(i), cols(h)]
                grad = dot_nt(v_ref[part(j), cols(h)], g_i)
                grads[part(j), :] = grad
                out = held[part(j), :]
                low = (out * kept[u]["inverse"]).astype(BF16)
                delta = jnp.sum(grad * out, axis=0, keepdims=True)
                kept[u]["delta"] = delta if j == 0 else kept[u]["delta"] + delta
                piece = dot_nn(low, g_i)
                if j == i:
                    vo[part(j), cols(h)] = piece
                    kept[u]["delta"] = kept[u]["delta"] * kept[u]["inverse"]
                    kept[u]["scaled"] = kept[u]["inverse"] * (1.0 - share(h, block))
                else:
                    vo[part(j), cols(h)] += piece
            return run

        return [raise_tile(j) for j in range(i + 1)] + [grad_tile(j) for j in range(i + 1)]

    def grads(u):
        h, i = units[u]
        held = s_buf.at[u % 3]
        grads = g_buf.at[u % 2]

        def tile(j):
            def run():
                q_i = q_ref[part(i), cols(h)]
                score = held[part(j), :] * ((grads[part(j), :] - kept[u]["delta"]) * kept[u]["scaled"])
                score = score.astype(BF16)
                piece = dot_nn(score, q_i)
                if j == i:
                    ko[part(j), cols(h)] = piece
                else:
                    ko[part(j), cols(h)] += piece
                turned = dot_nn(k_turned[h, :, part(j)], score)
                kept[u]["turned"] = turned if j == 0 else kept[u]["turned"] + turned
                if j == i:
                    qo[part(i), cols(h)] = kept[u]["turned"].T * scale
            return run

        return [tile(j) for j in range(i + 1)]

    def attend(at, *more):
        lists = [items for items in more if items]
        if 0 <= at - 2 < len(units):
            lists.append(grads(at - 2))
        if 0 <= at - 1 < len(units):
            lists.append(weights(at - 1))
        if 0 <= at < len(units):
            lists.append(scores(at))
        for run in merged(*lists):
            run()

    def memory_grads(h):
        hs = cols(h)
        held = {}

        def rows_of(i):
            def run():
                norm = norm_sum[0, h:h + 1, :]
                low = qf[part(i), hs]
                den = 1.0 + jnp.sum(low.astype(F32) * norm, axis=1, keepdims=True)
                inv = jnp.broadcast_to(1.0 / den, (block, size))
                inv_den[h, part(i), :] = inv
                num = g_ref[part(i), hs].astype(F32) * inv
                both = dot_tn(low, jnp.concatenate(split(num), axis=1))
                held["both"] = both if i == 0 else held["both"] + both
                if i == blocks - 1:
                    both = held["both"]
                    mem_src[1, 0, h] = (both[:, :size] + both[:, size:]) * share(h, size)
            return run

        return [rows_of(i) for i in range(blocks)]

    def read_memory(h):
        hs = cols(h)
        held = {}

        def rows_of(i):
            def run():
                memory_share = share(h, size)
                norm = norm_sum[0, h:h + 1, :]
                beside = jnp.concatenate(split(mem_sum[0, h]), axis=1)
                low = qf[part(i), hs].astype(F32)
                g_i = g_ref[part(i), hs]
                inv = inv_den[h, part(i), :]
                weighted = inv * memory_share
                turned = dot_nt(jnp.concatenate([g_i, g_i], axis=1), beside)
                product = jnp.sum(low * turned, axis=1, keepdims=True)
                den_grad = -(weighted * inv) * product
                row = jnp.sum(den_grad * low, axis=0, keepdims=True)
                held["row"] = row if i == 0 else held["row"] + row
                extra[part(i), hs] = (turned * weighted + den_grad * norm) * q_slope[part(i), hs]
                if i == blocks - 1:
                    norm_src[1, h:h + 1, :] = held["row"]
            return run

        return [rows_of(i) for i in range(blocks)]

    def memory_gate(h):
        both = jnp.sum(mem_sum[0, h] * mem_src[1, 0, h], axis=0, keepdims=True)
        gate_rows[h:h + 1, :] += both * (1.0 - share(h, size))

    def send_gates():
        if turns:
            hear(turns - 1)
        for other in range(1, n):
            gate_copy(other).start()
        gate_all[me] = gate_rows[...]

    def local_gate(h):
        held = {}

        def rows_of(i):
            def run():
                product = v_ref[part(i), cols(h)].astype(F32) * vo[part(i), cols(h)]
                row = jnp.sum(product, axis=0, keepdims=True)
                held["row"] = row if i == 0 else held["row"] + row
                if i == blocks - 1:
                    memory_share = share(h, size)
                    gate_rows[h:h + 1, :] -= held["row"] * (memory_share * (1.0 - memory_share))
            return run

        return [rows_of(i) for i in range(blocks)]

    def finish(h):
        hs = cols(h)
        local_share = 1.0 - share(h, size)
        high, rest = split(mem_sum[1, h])
        beside = jnp.concatenate([high, rest], axis=1)
        below = jnp.concatenate([high, rest], axis=0)
        for i in range(blocks):
            v_i = v_ref[part(i), hs]
            low = kf[part(i), hs]
            turned = dot_nt(jnp.concatenate([v_i, v_i], axis=1), beside)
            ko[part(i), hs] = ko[part(i), hs] * scale + turned * k_slope[part(i), hs]
            value = dot_nn(jnp.concatenate([low, low], axis=1), below)
            vo[part(i), hs] = vo[part(i), hs] * local_share + value
            qo[part(i), hs] += extra[part(i), hs]

    def key_memory(h):
        def run():
            mem_src[0, 0, h] = dot_tn(kf[:, cols(h)], v_ref[:, cols(h)])
        return [run]

    def query_features(h):
        def rows_of(i):
            def run():
                x = q_ref[part(i), cols(h)].astype(F32)
                flat = slope(x)
                q_slope[part(i), cols(h)] = flat
                qf[part(i), cols(h)] = (jnp.maximum(x, 0.0) + flat).astype(BF16)
            return run

        return [rows_of(i) for i in range(blocks)]

    turns = -(-(n - 1) // reach) - 1
    gate_rows[...] = jnp.zeros_like(gate_rows)
    norm_src[...] = jnp.zeros_like(norm_src)
    loads[0].wait()
    for h in range(heads):
        norm = jnp.zeros((1, size), F32)
        for i in range(blocks):
            x = k_ref[part(i), cols(h)].astype(F32)
            flat = slope(x)
            k_slope[part(i), cols(h)] = flat
            low = (jnp.maximum(x, 0.0) + flat).astype(BF16)
            kf[part(i), cols(h)] = low
            norm = norm + jnp.sum(low.astype(F32), axis=0, keepdims=True)
        norm_src[0, h:h + 1, :] = norm
    for i in (4, 5, 1, 2, 3):
        loads[i].wait()
    attend(-1, *(key_memory(h) for h in range(heads)), *(query_features(h) for h in range(heads)))
    pl.semaphore_wait(barrier, jnp.minimum(me, reach) + jnp.minimum(n - 1 - me, reach))
    send_norms(0)
    for h in range(heads):
        send_mem(0, 0, h)
    if turns:
        tell(0)

    last = len(units) + 1
    early = steps == 2 and heads == 3 and blocks == 4
    if early:
        polls = {6: [(0, 0, 0)], 8: [(0, 0, 1)], 9: [(0, 0, 2)], 10: [(0, 1, 0)], 11: [(0, 1, 1), (1, 0, 0)], 12: [(0, 1, 2)]}
        reads = {11: [0], 13: [1, 2]}
        late = [(1, 0, 1), (1, 0, 2)]
    else:
        polls, reads = {}, {}
        late = [(way, step, h) for step in range(steps - 1) for h in range(heads) for way in range(2)]
    begin = min(6, last - 1)
    for at in range(last + 1):
        parts = [memory_grads(at - begin)] if begin < at < begin + heads else []
        parts += [read_memory(h) for h in reads.get(at, [])]
        parts += [local_gate(h) for h in range(heads - 1) if at == (h + 1) * blocks + 1]
        attend(at, *parts)
        if begin < at < begin + heads:
            send_mem(1, 0, at - begin)
        if at == begin:
            take_norms(0)
            attend(-1, memory_grads(0))
            send_mem(1, 0, 0)
        for way, step, h in polls.get(at, []):
            take_mem(way, step, h)
            if (way, step) == (0, steps - 1):
                memory_gate(h)
        for turn in range(turns - 1):
            if at == min(7 + 2 * turn, last):
                hear(turn)
                tell(turn + 1)
        if at == last - 1:
            attend(-1, local_gate(heads - 1))
            if early:
                send_gates()
                take_mem(*late.pop(0))
    for h in range(last - begin + 1, heads):
        attend(-1, memory_grads(h))
        send_mem(1, 0, h)
    if early:
        send_norms(1)
    for way, step, h in late:
        take_mem(way, step, h)
    if not early:
        for h in range(heads):
            take_mem(0, steps - 1, h)
            memory_gate(h)
            attend(-1, read_memory(h))
        send_norms(1)
        send_gates()
    for h in range(heads):
        take_mem(1, steps - 1, h)
        finish(h)
    for way in range(2):
        for dist in range(1, reach + 1):
            @pl.when(can_send(way, dist))
            def _():
                norm_copy(way, dist).wait_send()
        for step in range(steps):
            @pl.when(can_send(way, 1 << step))
            def _():
                pltpu.make_async_copy(mem_src.at[way, step], mem_src.at[way, step], mem_send.at[way, step]).wait()
    take_norms(1)
    for h in range(heads):
        norm = norm_sum[1, h:h + 1, :]
        for i in range(blocks):
            ko[part(i), cols(h)] += norm * k_slope[part(i), cols(h)]
    others = gate_all.at[pl.ds(0, n - 1)]
    pltpu.make_async_copy(others, others, gate_recv).wait()
    gates = gate_all[0]
    for other in range(1, n):
        gates = gates + gate_all[other]
    gate_o[...] = gates
    pltpu.make_async_copy(others, others, gate_send).wait()


def write(heads, q_ref, k_ref, v_ref, gate_ref, q_hbm, k_hbm, v_hbm, gate_o, sems):
    copies = [
        pltpu.make_async_copy(source, target, sems.at[i])
        for i, (source, target) in enumerate(((q_ref, q_hbm), (k_ref, k_hbm), (v_ref, v_hbm)))
    ]
    for copy in copies:
        copy.start()
    for h in range(heads):
        gate_o[h] = jnp.sum(gate_ref[h:h + 1, :])
    for copy in copies:
        copy.wait()


def solution(mesh):
    n = mesh.shape["seq"]
    longest = max(n // 2, 2)
    steps = (longest - 1).bit_length()
    reach = longest - 1

    def per_device(queries, key_vectors, value_vectors, out_grad, gate_logit, doc_index):
        rows, width = queries.shape
        heads = gate_logit.shape[0]
        size = width // heads
        block = min(256, rows)
        wide = jax.ShapeDtypeStruct((rows, width), F32)
        vmem = pl.BlockSpec(memory_space=pltpu.VMEM)
        smem = pl.BlockSpec(memory_space=pltpu.SMEM)
        hbm = pl.BlockSpec(memory_space=pltpu.HBM)
        tall = -(-heads // 8) * 8
        dma = pltpu.SemaphoreType.DMA
        local = pl.pallas_call(
            functools.partial(kernel, n, steps, reach, heads, size, block),
            out_shape=(wide, wide, wide, jax.ShapeDtypeStruct((tall, size), F32)),
            in_specs=[hbm] * 6,
            out_specs=(vmem,) * 4,
            scratch_shapes=[
                pltpu.SMEM(doc_index.shape, jnp.int32),
                pltpu.SMEM(gate_logit.shape, F32),
                pltpu.VMEM((rows, width), BF16),
                pltpu.VMEM((rows, width), BF16),
                pltpu.VMEM((rows, width), BF16),
                pltpu.VMEM((rows, width), BF16),
                dma((6,)),
                pltpu.VMEM((rows, width), BF16),
                pltpu.VMEM((rows, width), BF16),
                pltpu.VMEM((rows, width), F32),
                pltpu.VMEM((rows, width), F32),
                pltpu.VMEM((rows, width), F32),
                pltpu.VMEM((heads, rows, size), F32),
                pltpu.VMEM((3, rows, block), F32),
                pltpu.VMEM((2, rows, block), F32),
                pltpu.VMEM((heads, size, rows), BF16),
                pltpu.VMEM((tall, size), F32),
                pltpu.VMEM((n, tall, size), F32),
                pltpu.VMEM((2, tall, size), F32),
                pltpu.VMEM((2, reach, tall, size), F32),
                pltpu.VMEM((2, tall, size), F32),
                pltpu.VMEM((2, steps, heads, size, size), F32),
                pltpu.VMEM((2, steps, heads, size, size), F32),
                pltpu.VMEM((2, heads, size, size), F32),
                dma((2, reach)),
                dma((2, reach)),
                dma((2, steps)),
                dma((2, steps, heads)),
                dma(()),
                dma(()),
                pltpu.SemaphoreType.REGULAR((max(-(-(n - 1) // reach) - 1, 1), 2)),
            ],
            compiler_params=pltpu.CompilerParams(
                collective_id=0, has_side_effects=True, vmem_limit_bytes=40 * 1024 * 1024
            ),
            cost_estimate=pl.CostEstimate(
                flops=14 * heads * rows * rows * size, bytes_accessed=20 * rows * width,
                transcendentals=heads * rows * rows,
            ),
            name="segment_backward",
        )(*(pltpu.with_memory_space_constraint(x, pltpu.HBM) for x in (doc_index, gate_logit, queries, key_vectors, value_vectors, out_grad)))
        return pl.pallas_call(
            functools.partial(write, heads),
            out_shape=(wide, wide, wide, jax.ShapeDtypeStruct((heads,), F32)),
            in_specs=[vmem] * 4,
            out_specs=(hbm, hbm, hbm, smem),
            scratch_shapes=[dma((3,))],
            compiler_params=pltpu.CompilerParams(vmem_limit_bytes=16 * 1024 * 1024),
            cost_estimate=pl.CostEstimate(
                flops=8 * rows * width * size, bytes_accessed=12 * rows * width,
                transcendentals=rows * width,
            ),
            name="segment_finish",
        )(*local)

    spec = P("seq", "head")
    return jax.shard_map(
        per_device, mesh=mesh, in_specs=(spec, spec, spec, spec, P("head"), P()),
        out_specs=(spec, spec, spec, P("head")), check_vma=False,
    )
```

```python
import functools
import math

import jax
import jax.numpy as jnp
from jax import lax
from jax.experimental import pallas as pl
from jax.experimental.pallas import tpu as pltpu
from jax.sharding import PartitionSpec as P

MESH = pl.DeviceIdType.MESH
F32 = jnp.float32
BF16 = jnp.bfloat16


def slope(x):
    return jnp.exp(jnp.minimum(x, 0.0))


def dot_nn(a, b):
    return lax.dot_general(a, b, (((1,), (0,)), ((), ())), preferred_element_type=F32)


def dot_nt(a, b):
    return lax.dot_general(a, b, (((1,), (1,)), ((), ())), preferred_element_type=F32)


def dot_tn(a, b):
    return lax.dot_general(a, b, (((0,), (0,)), ((), ())), preferred_element_type=F32)


def split(x):
    high = x.astype(BF16)
    return high, (x - high.astype(F32)).astype(BF16)


def merged(*lists):
    order = []
    for which, items in enumerate(lists):
        for at, item in enumerate(items):
            order.append(((at + 0.5) / len(items), which, at, item))
    return [entry[3] for entry in sorted(order, key=lambda entry: entry[:3])]


def kernel(
    n, steps, reach, heads, size, block,
    doc_hbm, logit_hbm, q_hbm, k_hbm, v_hbm, g_hbm,
    qo, ko, vo, gate_o, later_o, norm_o, share_o, k_slope, kf, held_ref,
    doc_ref, logit_ref, k_ref, load_sem,
    qf, q_slope, extra, inv_den, s_buf, g_buf, k_turned, gate_rows, gate_all,
    norm_src, norm_got, norm_sum, mem_src, mem_got, mem_sum,
    norm_send, norm_recv, mem_send, mem_recv, gate_send, gate_recv, entered,
):
    me = lax.axis_index("seq")
    v_ref, q_ref, g_ref = held_ref.at[0], held_ref.at[1], held_ref.at[2]
    rows = k_ref.shape[0]
    blocks = rows // block
    scale = size ** -0.5
    factor = scale * math.log2(math.e)
    signs = (1, -1)
    barrier = pltpu.get_barrier_semaphore()
    loads = [
        pltpu.make_async_copy(source, target, load_sem.at[i])
        for i, source, target in (
            (0, k_hbm, k_ref), (1, doc_hbm, doc_ref), (2, logit_hbm, logit_ref),
            (3, v_hbm, v_ref), (3, q_hbm, q_ref), (3, g_hbm, g_ref),
        )
    ]
    for load in loads:
        load.start()

    def peer(way, dist):
        return {"seq": lax.rem(me + signs[way] * dist + n, n)}

    def can_send(way, dist):
        return me + dist < n if way == 0 else me >= dist

    def can_recv(way, dist):
        return me >= dist if way == 0 else me + dist < n

    for dist in range(1, reach + 1):
        for way in range(2):
            @pl.when(can_send(way, dist))
            def _():
                pl.semaphore_signal(barrier, inc=1, device_id=peer(way, dist), device_id_type=MESH)

    def cols(h):
        return slice(h * size, (h + 1) * size)

    def part(i):
        return slice(i * block, (i + 1) * block)

    def share(h, width):
        return 1.0 / (1.0 + jnp.exp(-jnp.full((1, width), logit_ref[h], F32)))

    def weight(way, dist):
        other = lax.rem(me - signs[way] * dist + n, n)
        return jnp.where(doc_ref[other] == doc_ref[me], 1.0, 0.0).astype(F32)

    def norm_copy(way, dist):
        return pltpu.make_async_remote_copy(
            src_ref=norm_src.at[way], dst_ref=norm_got.at[way, dist - 1],
            send_sem=norm_send.at[way], recv_sem=norm_recv.at[way],
            device_id=peer(way, dist), device_id_type=MESH,
        )

    def mem_copy(way, step, h):
        return pltpu.make_async_remote_copy(
            src_ref=mem_src.at[way, step, h], dst_ref=mem_got.at[way, step, h],
            send_sem=mem_send.at[way], recv_sem=mem_recv.at[way, step, h],
            device_id=peer(way, 1 << step), device_id_type=MESH,
        )

    def gate_copy(other):
        return pltpu.make_async_remote_copy(
            src_ref=gate_rows, dst_ref=gate_all.at[me],
            send_sem=gate_send, recv_sem=gate_recv,
            device_id={"seq": lax.rem(me + other, n)}, device_id_type=MESH,
        )

    def tell(turn):
        for way in range(2):
            @pl.when(can_send(way, reach))
            def _():
                pl.semaphore_signal(entered.at[turn, way], inc=1, device_id=peer(way, reach), device_id_type=MESH)

    def hear(turn):
        for way in range(2):
            @pl.when(can_recv(way, reach))
            def _():
                pl.semaphore_wait(entered.at[turn, way], 1)

    def send_norms(way):
        for dist in range(1, reach + 1):
            @pl.when(can_send(way, dist))
            def _():
                norm_copy(way, dist).start()

    def behind(way):
        return me if way == 0 else n - 1 - me

    def wait_norms(way, count, sem):
        for some in range(1, reach + 1):
            @pl.when(jnp.minimum(count, reach) == some)
            def _():
                space = norm_got.at[way, pl.ds(0, some)]
                pltpu.make_async_copy(space, space, sem.at[way]).wait()

    def take_norms(way):
        norm_sum[way] = jnp.zeros_like(norm_sum[way])
        wait_norms(way, behind(way), norm_recv)
        for dist in range(1, reach + 1):
            @pl.when(can_recv(way, dist))
            def _():
                norm_sum[way] += weight(way, dist) * norm_got[way, dist - 1]

    def send_mem(way, step, h):
        @pl.when(can_send(way, 1 << step))
        def _():
            mem_copy(way, step, h).start()

    def take_mem(way, step, h):
        if step == 0:
            mem_sum[way, h] = jnp.zeros_like(mem_sum[way, h])

        @pl.when(can_recv(way, 1 << step))
        def _():
            mem_copy(way, step, h).wait_recv()
            mem_sum[way, h] += weight(way, 1 << step) * mem_got[way, step, h]

        if step + 1 < steps:
            mem_src[way, step + 1, h] = mem_src[way, 0, h] + mem_sum[way, h]
            send_mem(way, step + 1, h)

    units = [(h, i) for h in range(heads) for i in range(blocks)]
    kept = [{} for _ in units]

    def scores(u):
        h, i = units[u]
        held = s_buf.at[u % 3]

        def tile(j):
            def run():
                if i == 0:
                    k_turned[h] = k_ref[:, cols(h)].T
                out = dot_nt(k_ref[part(j), cols(h)], q_ref[part(i), cols(h)])
                if j == i:
                    key_ids = lax.broadcasted_iota(jnp.int32, (block, block), 0)
                    query_ids = lax.broadcasted_iota(jnp.int32, (block, block), 1)
                    out = jnp.where(key_ids <= query_ids, out, -1e30)
                held[part(j), :] = out
                top = jnp.max(out, axis=0, keepdims=True)
                kept[u]["top"] = top if j == 0 else jnp.maximum(kept[u]["top"], top)
            return run

        return [tile(j) for j in range(i + 1)]

    def weights(u):
        h, i = units[u]
        held = s_buf.at[u % 3]
        grads = g_buf.at[u % 2]

        def raise_tile(j):
            def run():
                out = jnp.exp2((held[part(j), :] - kept[u]["top"]) * factor)
                held[part(j), :] = out
                total = jnp.sum(out, axis=0, keepdims=True)
                kept[u]["total"] = total if j == 0 else kept[u]["total"] + total
                if j == i:
                    kept[u]["inverse"] = 1.0 / kept[u]["total"]
            return run

        def grad_tile(j):
            def run():
                g_i = g_ref[part(i), cols(h)]
                grad = dot_nt(v_ref[part(j), cols(h)], g_i)
                grads[part(j), :] = grad
                out = held[part(j), :]
                low = (out * kept[u]["inverse"]).astype(BF16)
                delta = jnp.sum(grad * out, axis=0, keepdims=True)
                kept[u]["delta"] = delta if j == 0 else kept[u]["delta"] + delta
                piece = dot_nn(low, g_i)
                if j == i:
                    vo[part(j), cols(h)] = piece
                    kept[u]["delta"] = kept[u]["delta"] * kept[u]["inverse"]
                    kept[u]["scaled"] = kept[u]["inverse"] * (1.0 - share(h, block))
                else:
                    vo[part(j), cols(h)] += piece
            return run

        return [raise_tile(j) for j in range(i + 1)] + [grad_tile(j) for j in range(i + 1)]

    def grads(u):
        h, i = units[u]
        held = s_buf.at[u % 3]
        grads = g_buf.at[u % 2]

        def tile(j):
            def run():
                q_i = q_ref[part(i), cols(h)]
                score = held[part(j), :] * ((grads[part(j), :] - kept[u]["delta"]) * kept[u]["scaled"])
                score = score.astype(BF16)
                piece = dot_nn(score, q_i)
                if j == i:
                    ko[part(j), cols(h)] = piece
                else:
                    ko[part(j), cols(h)] += piece
                turned = dot_nn(k_turned[h, :, part(j)], score)
                kept[u]["turned"] = turned if j == 0 else kept[u]["turned"] + turned
                if j == i:
                    qo[part(i), cols(h)] = kept[u]["turned"].T * scale
            return run

        return [tile(j) for j in range(i + 1)]

    def attend(at, *more):
        lists = [items for items in more if items]
        if 0 <= at - 2 < len(units):
            lists.append(grads(at - 2))
        if 0 <= at - 1 < len(units):
            lists.append(weights(at - 1))
        if 0 <= at < len(units):
            lists.append(scores(at))
        for run in merged(*lists):
            run()

    def memory_grads(h):
        hs = cols(h)
        held = {}

        def rows_of(i):
            def run():
                norm = norm_sum[0, h:h + 1, :]
                low = qf[part(i), hs]
                den = 1.0 + jnp.sum(low.astype(F32) * norm, axis=1, keepdims=True)
                inv = jnp.broadcast_to(1.0 / den, (block, size))
                inv_den[h, part(i), :] = inv
                num = g_ref[part(i), hs].astype(F32) * inv
                both = dot_tn(low, jnp.concatenate(split(num), axis=1))
                held["both"] = both if i == 0 else held["both"] + both
                if i == blocks - 1:
                    both = held["both"]
                    mem_src[1, 0, h] = (both[:, :size] + both[:, size:]) * share(h, size)
            return run

        return [rows_of(i) for i in range(blocks)]

    def read_memory(h):
        hs = cols(h)
        held = {}

        def rows_of(i):
            def run():
                memory_share = share(h, size)
                norm = norm_sum[0, h:h + 1, :]
                beside = jnp.concatenate(split(mem_sum[0, h]), axis=1)
                low = qf[part(i), hs].astype(F32)
                g_i = g_ref[part(i), hs]
                inv = inv_den[h, part(i), :]
                weighted = inv * memory_share
                turned = dot_nt(jnp.concatenate([g_i, g_i], axis=1), beside)
                product = jnp.sum(low * turned, axis=1, keepdims=True)
                den_grad = -(weighted * inv) * product
                row = jnp.sum(den_grad * low, axis=0, keepdims=True)
                held["row"] = row if i == 0 else held["row"] + row
                extra[part(i), hs] = (turned * weighted + den_grad * norm) * q_slope[part(i), hs]
                if i == blocks - 1:
                    norm_src[1, h:h + 1, :] = held["row"]
            return run

        return [rows_of(i) for i in range(blocks)]

    def memory_gate(h):
        both = jnp.sum(mem_sum[0, h] * mem_src[1, 0, h], axis=0, keepdims=True)
        gate_rows[h:h + 1, :] += both * (1.0 - share(h, size))

    def send_gates():
        if turns:
            hear(turns - 1)
        for other in range(1, n):
            gate_copy(other).start()
        gate_all[me] = gate_rows[...]

    def local_gate(h):
        held = {}

        def rows_of(i):
            def run():
                product = v_ref[part(i), cols(h)].astype(F32) * vo[part(i), cols(h)]
                row = jnp.sum(product, axis=0, keepdims=True)
                held["row"] = row if i == 0 else held["row"] + row
                if i == blocks - 1:
                    memory_share = share(h, size)
                    gate_rows[h:h + 1, :] -= held["row"] * (memory_share * (1.0 - memory_share))
            return run

        return [rows_of(i) for i in range(blocks)]

    def add_extra(h):
        for i in range(blocks):
            qo[part(i), cols(h)] += extra[part(i), cols(h)]

    def finish(h):
        hs = cols(h)
        local_share = 1.0 - share(h, size)
        high, rest = split(mem_sum[1, h])
        beside = jnp.concatenate([high, rest], axis=1)
        below = jnp.concatenate([high, rest], axis=0)
        for i in range(blocks):
            v_i = v_ref[part(i), hs]
            low = kf[part(i), hs]
            turned = dot_nt(jnp.concatenate([v_i, v_i], axis=1), beside)
            ko[part(i), hs] = ko[part(i), hs] * scale + turned * k_slope[part(i), hs]
            value = dot_nn(jnp.concatenate([low, low], axis=1), below)
            vo[part(i), hs] = vo[part(i), hs] * local_share + value

    def key_memory(h):
        def run():
            mem_src[0, 0, h] = dot_tn(kf[:, cols(h)], v_ref[:, cols(h)])
        return [run]

    def query_features(h):
        def rows_of(i):
            def run():
                x = q_ref[part(i), cols(h)].astype(F32)
                flat = slope(x)
                q_slope[part(i), cols(h)] = flat
                qf[part(i), cols(h)] = (jnp.maximum(x, 0.0) + flat).astype(BF16)
            return run

        return [rows_of(i) for i in range(blocks)]

    turns = -(-(n - 1) // reach) - 1
    gate_rows[...] = jnp.zeros_like(gate_rows)
    norm_src[...] = jnp.zeros_like(norm_src)
    loads[0].wait()
    for h in range(heads):
        norm = jnp.zeros((1, size), F32)
        for i in range(blocks):
            x = k_ref[part(i), cols(h)].astype(F32)
            flat = slope(x)
            k_slope[part(i), cols(h)] = flat
            low = (jnp.maximum(x, 0.0) + flat).astype(BF16)
            kf[part(i), cols(h)] = low
            norm = norm + jnp.sum(low.astype(F32), axis=0, keepdims=True)
        norm_src[0, h:h + 1, :] = norm
    loads[1].wait()
    loads[2].wait()
    pltpu.make_async_copy(held_ref, held_ref, load_sem.at[3]).wait()
    attend(-1, *(key_memory(h) for h in range(heads)), *(query_features(h) for h in range(heads)))
    pl.semaphore_wait(barrier, jnp.minimum(me, reach) + jnp.minimum(n - 1 - me, reach))
    send_norms(0)
    for h in range(heads):
        send_mem(0, 0, h)
    if turns:
        tell(0)

    last = len(units) + 1
    early = steps == 2 and heads == 3 and blocks == 4
    if early:
        polls = {6: [(0, 0, 0)], 7: [(0, 0, 1)], 8: [(0, 0, 2)], 11: [(0, 1, 0), (1, 0, 0)], 12: [(0, 1, 1), (0, 1, 2)]}
        reads = {13: [0, 1, 2]}
        late = [(1, 0, 1), (1, 0, 2)]
    else:
        polls, reads = {}, {}
        late = [(way, step, h) for step in range(steps - 1) for h in range(heads) for way in range(2)]
    begin = min(6, last - 1)
    for at in range(last + 1):
        parts = [memory_grads(at - begin)] if begin < at < begin + heads else []
        parts += [read_memory(h) for h in reads.get(at, [])]
        parts += [local_gate(h) for h in range(heads - 1) if at == (h + 1) * blocks + 1]
        attend(at, *parts)
        if begin < at < begin + heads:
            send_mem(1, 0, at - begin)
        if at == begin:
            take_norms(0)
            attend(-1, memory_grads(0))
            send_mem(1, 0, 0)
        if at == last - 1:
            attend(-1, local_gate(heads - 1))
        for way, step, h in polls.get(at, []):
            take_mem(way, step, h)
            if (way, step) == (0, steps - 1):
                memory_gate(h)
        for turn in range(turns - 1):
            if at == min(7 + 2 * turn, last):
                hear(turn)
                tell(turn + 1)
        if at == last - 1 and early:
            send_gates()
            way, step, h = late.pop(0)
            take_mem(way, step, h)
    for h in range(last - begin + 1, heads):
        attend(-1, memory_grads(h))
        send_mem(1, 0, h)
    if early:
        send_norms(1)
    for way, step, h in late:
        take_mem(way, step, h)
    if not early:
        for h in range(heads):
            take_mem(0, steps - 1, h)
            memory_gate(h)
            attend(-1, read_memory(h))
        send_norms(1)
        send_gates()
    for h in range(heads):
        add_extra(h)
    share_o[...] = jnp.broadcast_to(1.0 - share(heads - 1, size), share_o.shape)
    for h in range(heads - 1):
        take_mem(1, steps - 1, h)
        finish(h)
    for way in range(2):
        ahead = behind(1 - way)
        wait_norms(way, ahead, norm_send)
        for some in range(1, steps + 1):
            @pl.when((ahead >= 1 << (some - 1)) & ((ahead < 1 << some) | (some == steps)))
            def _():
                space = mem_src.at[way, pl.ds(0, some)]
                pltpu.make_async_copy(space, space, mem_send.at[way]).wait()
    take_mem(1, steps - 1, heads - 1)
    later_o[...] = mem_sum[1, heads - 1]
    take_norms(1)
    norm_o[...] = norm_sum[1]
    others = gate_all.at[pl.ds(0, n - 1)]
    pltpu.make_async_copy(others, others, gate_recv).wait()
    gates = gate_all[0]
    for other in range(1, n):
        gates = gates + gate_all[other]
    gate_o[...] = gates
    pltpu.make_async_copy(others, others, gate_send).wait()


def write(
    heads, size, block,
    q_ref, k_ref, v_ref, gate_ref, later_ref, norm_ref, share_ref, slope_ref, kf_ref, held_ref,
    q_hbm, k_hbm, v_hbm, gate_o, k_out, v_out, sems,
):
    rows = q_ref.shape[0]
    ready = (heads - 1) * size
    front, back = slice(0, ready), slice(ready, ready + size)
    copies = []

    def send(source, target):
        copies.append(pltpu.make_async_copy(source, target, sems.at[len(copies)]))
        copies[-1].start()

    send(q_ref, q_hbm)
    if ready:
        send(v_ref.at[:, front], v_hbm.at[:, front])
        for h in range(heads - 1):
            hs = slice(h * size, (h + 1) * size)
            for i in range(rows // block):
                here = slice(i * block, (i + 1) * block)
                k_out[here, hs] = k_ref[here, hs] + norm_ref[h:h + 1, :] * slope_ref[here, hs]
        send(k_out.at[:, front], k_hbm.at[:, front])
    high, rest = split(later_ref[...])
    beside = jnp.concatenate([high, rest], axis=1)
    below = jnp.concatenate([high, rest], axis=0)
    for i in range(rows // block):
        here = slice(i * block, (i + 1) * block)
        v_i = held_ref[0, here, back]
        low = kf_ref[here, back]
        turned = dot_nt(jnp.concatenate([v_i, v_i], axis=1), beside) + norm_ref[heads - 1:heads, :]
        k_out[here, back] = k_ref[here, back] * size ** -0.5 + turned * slope_ref[here, back]
        value = dot_nn(jnp.concatenate([low, low], axis=1), below)
        v_out[here, :] = v_ref[here, back] * share_ref[0:1, :] + value
    send(k_out.at[:, back], k_hbm.at[:, back])
    send(v_out, v_hbm.at[:, back])
    for h in range(heads):
        gate_o[h] = jnp.sum(gate_ref[h:h + 1, :])
    for copy in copies:
        copy.wait()


def solution(mesh):
    n = mesh.shape["seq"]
    longest = max(n // 2, 2)
    steps = (longest - 1).bit_length()
    reach = longest - 1

    def per_device(queries, key_vectors, value_vectors, out_grad, gate_logit, doc_index):
        rows, width = queries.shape
        heads = gate_logit.shape[0]
        size = width // heads
        block = min(256, rows)
        wide = jax.ShapeDtypeStruct((rows, width), F32)
        vmem = pl.BlockSpec(memory_space=pltpu.VMEM)
        smem = pl.BlockSpec(memory_space=pltpu.SMEM)
        hbm = pl.BlockSpec(memory_space=pltpu.HBM)
        tall = -(-heads // 8) * 8
        dma = pltpu.SemaphoreType.DMA
        small = jax.ShapeDtypeStruct((tall, size), F32)
        local = pl.pallas_call(
            functools.partial(kernel, n, steps, reach, heads, size, block),
            out_shape=(
                wide, wide, wide, small, jax.ShapeDtypeStruct((size, size), F32), small, small, wide,
                jax.ShapeDtypeStruct((rows, width), BF16), jax.ShapeDtypeStruct((3, rows, width), BF16),
            ),
            in_specs=[hbm] * 6,
            out_specs=(vmem,) * 10,
            scratch_shapes=[
                pltpu.SMEM(doc_index.shape, jnp.int32),
                pltpu.SMEM(gate_logit.shape, F32),
                pltpu.VMEM((rows, width), BF16),
                dma((4,)),
                pltpu.VMEM((rows, width), BF16),
                pltpu.VMEM((rows, width), F32),
                pltpu.VMEM((rows, width), F32),
                pltpu.VMEM((heads, rows, size), F32),
                pltpu.VMEM((3, rows, block), F32),
                pltpu.VMEM((2, rows, block), F32),
                pltpu.VMEM((heads, size, rows), BF16),
                pltpu.VMEM((tall, size), F32),
                pltpu.VMEM((n, tall, size), F32),
                pltpu.VMEM((2, tall, size), F32),
                pltpu.VMEM((2, reach, tall, size), F32),
                pltpu.VMEM((2, tall, size), F32),
                pltpu.VMEM((2, steps, heads, size, size), F32),
                pltpu.VMEM((2, steps, heads, size, size), F32),
                pltpu.VMEM((2, heads, size, size), F32),
                dma((2,)),
                dma((2,)),
                dma((2,)),
                dma((2, steps, heads)),
                dma(()),
                dma(()),
                pltpu.SemaphoreType.REGULAR((max(-(-(n - 1) // reach) - 1, 1), 2)),
            ],
            compiler_params=pltpu.CompilerParams(
                collective_id=0, has_side_effects=True, vmem_limit_bytes=40 * 1024 * 1024
            ),
            cost_estimate=pl.CostEstimate(
                flops=14 * heads * rows * rows * size, bytes_accessed=20 * rows * width,
                transcendentals=heads * rows * rows,
            ),
            name="segment_backward",
        )(*(pltpu.with_memory_space_constraint(x, pltpu.HBM) for x in (doc_index, gate_logit, queries, key_vectors, value_vectors, out_grad)))
        return pl.pallas_call(
            functools.partial(write, heads, size, block),
            out_shape=(wide, wide, wide, jax.ShapeDtypeStruct((heads,), F32)),
            in_specs=[vmem] * 10,
            out_specs=(hbm, hbm, hbm, smem),
            scratch_shapes=[pltpu.VMEM((rows, width), F32), pltpu.VMEM((rows, size), F32), dma((5,))],
            compiler_params=pltpu.CompilerParams(vmem_limit_bytes=16 * 1024 * 1024),
            cost_estimate=pl.CostEstimate(
                flops=8 * rows * width * size, bytes_accessed=12 * rows * width,
                transcendentals=rows * width,
            ),
            name="segment_finish",
        )(*local)

    spec = P("seq", "head")
    return jax.shard_map(
        per_device, mesh=mesh, in_specs=(spec, spec, spec, spec, P("head"), P()),
        out_specs=(spec, spec, spec, P("head")), check_vma=False,
    )
```

```python
import functools
import math

import jax
import jax.numpy as jnp
from jax import lax
from jax.experimental import pallas as pl
from jax.experimental.pallas import tpu as pltpu
from jax.sharding import PartitionSpec as P

MESH = pl.DeviceIdType.MESH
F32 = jnp.float32
BF16 = jnp.bfloat16


def slope(x):
    return jnp.exp(jnp.minimum(x, 0.0))


def dot_nn(a, b):
    return lax.dot_general(a, b, (((1,), (0,)), ((), ())), preferred_element_type=F32)


def dot_nt(a, b):
    return lax.dot_general(a, b, (((1,), (1,)), ((), ())), preferred_element_type=F32)


def dot_tn(a, b):
    return lax.dot_general(a, b, (((0,), (0,)), ((), ())), preferred_element_type=F32)


def split(x):
    high = x.astype(BF16)
    return high, (x - high.astype(F32)).astype(BF16)


def merged(*lists):
    order = []
    for which, items in enumerate(lists):
        for at, item in enumerate(items):
            order.append(((at + 0.5) / len(items), which, at, item))
    return [entry[3] for entry in sorted(order, key=lambda entry: entry[:3])]


def kernel(
    n, steps, reach, heads, size, block,
    doc_hbm, logit_hbm, q_hbm, k_hbm, v_hbm, g_hbm,
    qo, ko, vo, gate_o, later_o, norm_o, share_o, k_slope, kf, held_ref,
    doc_ref, logit_ref, k_ref, load_sem,
    qf, q_slope, extra, inv_den, s_buf, g_buf, k_turned, gate_rows, gate_all,
    norm_src, norm_got, norm_sum, mem_src, mem_got, mem_sum,
    norm_send, norm_recv, mem_send, mem_recv, gate_send, gate_recv, entered,
):
    me = lax.axis_index("seq")
    v_ref, q_ref, g_ref = held_ref.at[0], held_ref.at[1], held_ref.at[2]
    rows = k_ref.shape[0]
    blocks = rows // block
    scale = size ** -0.5
    factor = scale * math.log2(math.e)
    signs = (1, -1)
    barrier = pltpu.get_barrier_semaphore()
    loads = [
        pltpu.make_async_copy(source, target, load_sem.at[i])
        for i, source, target in (
            (0, k_hbm, k_ref), (1, doc_hbm, doc_ref), (2, logit_hbm, logit_ref),
            (3, v_hbm, v_ref), (3, q_hbm, q_ref), (3, g_hbm, g_ref),
        )
    ]
    for load in loads:
        load.start()

    def peer(way, dist):
        return {"seq": lax.rem(me + signs[way] * dist + n, n)}

    def can_send(way, dist):
        return me + dist < n if way == 0 else me >= dist

    def can_recv(way, dist):
        return me >= dist if way == 0 else me + dist < n

    for dist in range(1, reach + 1):
        for way in range(2):
            @pl.when(can_send(way, dist))
            def _():
                pl.semaphore_signal(barrier, inc=1, device_id=peer(way, dist), device_id_type=MESH)

    def cols(h):
        return slice(h * size, (h + 1) * size)

    def part(i):
        return slice(i * block, (i + 1) * block)

    def share(h, width):
        return 1.0 / (1.0 + jnp.exp(-jnp.full((1, width), logit_ref[h], F32)))

    def weight(way, dist):
        other = lax.rem(me - signs[way] * dist + n, n)
        return jnp.where(doc_ref[other] == doc_ref[me], 1.0, 0.0).astype(F32)

    def norm_copy(way, dist):
        return pltpu.make_async_remote_copy(
            src_ref=norm_src.at[way], dst_ref=norm_got.at[way, dist - 1],
            send_sem=norm_send.at[way], recv_sem=norm_recv.at[way],
            device_id=peer(way, dist), device_id_type=MESH,
        )

    def mem_copy(way, step, h):
        return pltpu.make_async_remote_copy(
            src_ref=mem_src.at[way, step, h], dst_ref=mem_got.at[way, step, h],
            send_sem=mem_send.at[way], recv_sem=mem_recv.at[way, step, h],
            device_id=peer(way, 1 << step), device_id_type=MESH,
        )

    def gate_copy(other):
        return pltpu.make_async_remote_copy(
            src_ref=gate_rows, dst_ref=gate_all.at[me],
            send_sem=gate_send, recv_sem=gate_recv,
            device_id={"seq": lax.rem(me + other, n)}, device_id_type=MESH,
        )

    def tell(turn):
        for way in range(2):
            @pl.when(can_send(way, reach))
            def _():
                pl.semaphore_signal(entered.at[turn, way], inc=1, device_id=peer(way, reach), device_id_type=MESH)

    def hear(turn):
        for way in range(2):
            @pl.when(can_recv(way, reach))
            def _():
                pl.semaphore_wait(entered.at[turn, way], 1)

    def send_norms(way):
        for dist in range(1, reach + 1):
            @pl.when(can_send(way, dist))
            def _():
                norm_copy(way, dist).start()

    def behind(way):
        return me if way == 0 else n - 1 - me

    def wait_norms(way, count, sem):
        for some in range(1, reach + 1):
            @pl.when(jnp.minimum(count, reach) == some)
            def _():
                space = norm_got.at[way, pl.ds(0, some)]
                pltpu.make_async_copy(space, space, sem.at[way]).wait()

    def take_norms(way):
        norm_sum[way] = jnp.zeros_like(norm_sum[way])
        wait_norms(way, behind(way), norm_recv)
        for dist in range(1, reach + 1):
            @pl.when(can_recv(way, dist))
            def _():
                norm_sum[way] += weight(way, dist) * norm_got[way, dist - 1]

    def send_mem(way, step, h):
        @pl.when(can_send(way, 1 << step))
        def _():
            mem_copy(way, step, h).start()

    def take_mem(way, step, h):
        if step == 0:
            mem_sum[way, h] = jnp.zeros_like(mem_sum[way, h])

        @pl.when(can_recv(way, 1 << step))
        def _():
            mem_copy(way, step, h).wait_recv()
            mem_sum[way, h] += weight(way, 1 << step) * mem_got[way, step, h]

        if step + 1 < steps:
            mem_src[way, step + 1, h] = mem_src[way, 0, h] + mem_sum[way, h]
            send_mem(way, step + 1, h)

    units = [(h, i) for h in range(heads) for i in range(blocks)]
    kept = [{} for _ in units]

    def scores(u):
        h, i = units[u]
        held = s_buf.at[u % 3]

        def tile(j):
            def run():
                if i == 0:
                    k_turned[h] = k_ref[:, cols(h)].T
                out = dot_nt(k_ref[part(j), cols(h)], q_ref[part(i), cols(h)])
                if j == i:
                    key_ids = lax.broadcasted_iota(jnp.int32, (block, block), 0)
                    query_ids = lax.broadcasted_iota(jnp.int32, (block, block), 1)
                    out = jnp.where(key_ids <= query_ids, out, -1e30)
                held[part(j), :] = out
                top = jnp.max(out, axis=0, keepdims=True)
                kept[u]["top"] = top if j == 0 else jnp.maximum(kept[u]["top"], top)
            return run

        return [tile(j) for j in range(i + 1)]

    def weights(u):
        h, i = units[u]
        held = s_buf.at[u % 3]
        grads = g_buf.at[u % 2]

        def raise_tile(j):
            def run():
                out = jnp.exp2((held[part(j), :] - kept[u]["top"]) * factor)
                held[part(j), :] = out
                total = jnp.sum(out, axis=0, keepdims=True)
                kept[u]["total"] = total if j == 0 else kept[u]["total"] + total
                if j == i:
                    kept[u]["inverse"] = 1.0 / kept[u]["total"]
            return run

        def grad_tile(j):
            def run():
                g_i = g_ref[part(i), cols(h)]
                grad = dot_nt(v_ref[part(j), cols(h)], g_i)
                grads[part(j), :] = grad
                out = held[part(j), :]
                low = (out * kept[u]["inverse"]).astype(BF16)
                delta = jnp.sum(grad * out, axis=0, keepdims=True)
                kept[u]["delta"] = delta if j == 0 else kept[u]["delta"] + delta
                piece = dot_nn(low, g_i)
                if j == i:
                    vo[part(j), cols(h)] = piece
                    kept[u]["delta"] = kept[u]["delta"] * kept[u]["inverse"]
                    kept[u]["scaled"] = kept[u]["inverse"] * (1.0 - share(h, block))
                else:
                    vo[part(j), cols(h)] += piece
            return run

        return [raise_tile(j) for j in range(i + 1)] + [grad_tile(j) for j in range(i + 1)]

    def grads(u):
        h, i = units[u]
        held = s_buf.at[u % 3]
        grads = g_buf.at[u % 2]

        def tile(j):
            def run():
                q_i = q_ref[part(i), cols(h)]
                score = held[part(j), :] * ((grads[part(j), :] - kept[u]["delta"]) * kept[u]["scaled"])
                score = score.astype(BF16)
                piece = dot_nn(score, q_i)
                if j == i:
                    ko[part(j), cols(h)] = piece
                else:
                    ko[part(j), cols(h)] += piece
                turned = dot_nn(k_turned[h, :, part(j)], score)
                kept[u]["turned"] = turned if j == 0 else kept[u]["turned"] + turned
                if j == i:
                    qo[part(i), cols(h)] = kept[u]["turned"].T * scale
            return run

        return [tile(j) for j in range(i + 1)]

    def attend(at, *more):
        lists = [items for items in more if items]
        if 0 <= at - 2 < len(units):
            lists.append(grads(at - 2))
        if 0 <= at - 1 < len(units):
            lists.append(weights(at - 1))
        if 0 <= at < len(units):
            lists.append(scores(at))
        for run in merged(*lists):
            run()

    def memory_grads(h):
        hs = cols(h)
        held = {}

        def rows_of(i):
            def run():
                norm = norm_sum[0, h:h + 1, :]
                low = qf[part(i), hs]
                den = 1.0 + jnp.sum(low.astype(F32) * norm, axis=1, keepdims=True)
                inv = jnp.broadcast_to(1.0 / den, (block, size))
                inv_den[h, part(i), :] = inv
                num = g_ref[part(i), hs].astype(F32) * inv
                both = dot_tn(low, jnp.concatenate(split(num), axis=1))
                held["both"] = both if i == 0 else held["both"] + both
                if i == blocks - 1:
                    both = held["both"]
                    mem_src[1, 0, h] = (both[:, :size] + both[:, size:]) * share(h, size)
            return run

        return [rows_of(i) for i in range(blocks)]

    def read_memory(h):
        hs = cols(h)
        held = {}

        def rows_of(i):
            def run():
                memory_share = share(h, size)
                norm = norm_sum[0, h:h + 1, :]
                beside = jnp.concatenate(split(mem_sum[0, h]), axis=1)
                low = qf[part(i), hs].astype(F32)
                g_i = g_ref[part(i), hs]
                inv = inv_den[h, part(i), :]
                weighted = inv * memory_share
                turned = dot_nt(jnp.concatenate([g_i, g_i], axis=1), beside)
                product = jnp.sum(low * turned, axis=1, keepdims=True)
                den_grad = -(weighted * inv) * product
                row = jnp.sum(den_grad * low, axis=0, keepdims=True)
                held["row"] = row if i == 0 else held["row"] + row
                extra[part(i), hs] = (turned * weighted + den_grad * norm) * q_slope[part(i), hs]
                if i == blocks - 1:
                    norm_src[1, h:h + 1, :] = held["row"]
            return run

        return [rows_of(i) for i in range(blocks)]

    def memory_gate(h):
        both = jnp.sum(mem_sum[0, h] * mem_src[1, 0, h], axis=0, keepdims=True)
        gate_rows[h:h + 1, :] += both * (1.0 - share(h, size))

    def send_gates():
        if turns:
            hear(turns - 1)
        for other in range(1, n):
            gate_copy(other).start()
        gate_all[me] = gate_rows[...]

    def local_gate(h):
        held = {}

        def rows_of(i):
            def run():
                product = v_ref[part(i), cols(h)].astype(F32) * vo[part(i), cols(h)]
                row = jnp.sum(product, axis=0, keepdims=True)
                held["row"] = row if i == 0 else held["row"] + row
                if i == blocks - 1:
                    memory_share = share(h, size)
                    gate_rows[h:h + 1, :] -= held["row"] * (memory_share * (1.0 - memory_share))
            return run

        return [rows_of(i) for i in range(blocks)]

    def add_extra(h):
        for i in range(blocks):
            qo[part(i), cols(h)] += extra[part(i), cols(h)]

    def finish(h):
        hs = cols(h)
        local_share = 1.0 - share(h, size)
        high, rest = split(mem_sum[1, h])
        beside = jnp.concatenate([high, rest], axis=1)
        below = jnp.concatenate([high, rest], axis=0)
        for i in range(blocks):
            v_i = v_ref[part(i), hs]
            low = kf[part(i), hs]
            turned = dot_nt(jnp.concatenate([v_i, v_i], axis=1), beside)
            ko[part(i), hs] = ko[part(i), hs] * scale + turned * k_slope[part(i), hs]
            value = dot_nn(jnp.concatenate([low, low], axis=1), below)
            vo[part(i), hs] = vo[part(i), hs] * local_share + value

    def key_memory(h):
        def run():
            mem_src[0, 0, h] = dot_tn(kf[:, cols(h)], v_ref[:, cols(h)])
        return [run]

    def query_features(h):
        def rows_of(i):
            def run():
                x = q_ref[part(i), cols(h)].astype(F32)
                flat = slope(x)
                q_slope[part(i), cols(h)] = flat
                qf[part(i), cols(h)] = (jnp.maximum(x, 0.0) + flat).astype(BF16)
            return run

        return [rows_of(i) for i in range(blocks)]

    turns = -(-(n - 1) // reach) - 1
    gate_rows[...] = jnp.zeros_like(gate_rows)
    norm_src[...] = jnp.zeros_like(norm_src)
    loads[0].wait()
    for h in range(heads):
        norm = jnp.zeros((1, size), F32)
        for i in range(blocks):
            x = k_ref[part(i), cols(h)].astype(F32)
            flat = slope(x)
            k_slope[part(i), cols(h)] = flat
            low = (jnp.maximum(x, 0.0) + flat).astype(BF16)
            kf[part(i), cols(h)] = low
            norm = norm + jnp.sum(low.astype(F32), axis=0, keepdims=True)
        norm_src[0, h:h + 1, :] = norm
    loads[1].wait()
    loads[2].wait()
    pltpu.make_async_copy(held_ref, held_ref, load_sem.at[3]).wait()
    attend(-1, *(key_memory(h) for h in range(heads)), *(query_features(h) for h in range(heads)))
    pl.semaphore_wait(barrier, jnp.minimum(me, reach) + jnp.minimum(n - 1 - me, reach))
    send_norms(0)
    for h in range(heads):
        send_mem(0, 0, h)
    if turns:
        tell(0)

    last = len(units) + 1
    early = steps == 2 and heads == 3 and blocks == 4
    if early:
        polls = {6: [(0, 0, 0)], 7: [(0, 0, 1)], 8: [(0, 0, 2)], 11: [(0, 1, 0), (1, 0, 0)], 12: [(0, 1, 1), (0, 1, 2)]}
        reads, late = {}, []
    else:
        polls, reads = {}, {}
        late = [(way, step, h) for step in range(steps - 1) for h in range(heads) for way in range(2)]
    begin = min(6, last - 1)
    for at in range(last + 1):
        parts = [memory_grads(at - begin)] if begin < at < begin + heads else []
        parts += [read_memory(h) for h in reads.get(at, [])]
        parts += [local_gate(h) for h in range(heads - 1) if at == (h + 1) * blocks + 1]
        attend(at, *parts)
        if begin < at < begin + heads:
            send_mem(1, 0, at - begin)
        if at == begin:
            take_norms(0)
            attend(-1, memory_grads(0))
            for way, step, h in polls.pop(at, []):
                take_mem(way, step, h)
            send_mem(1, 0, 0)
        if at == last - 1:
            attend(-1, local_gate(heads - 1))
        for way, step, h in polls.get(at, []):
            take_mem(way, step, h)
            if (way, step) == (0, steps - 1):
                memory_gate(h)
        for turn in range(turns - 1):
            if at == min(7 + 2 * turn, last):
                hear(turn)
                tell(turn + 1)
        if at == last - 1 and early:
            send_gates()
            take_mem(1, 0, 1)
            attend(-1, *(read_memory(h) for h in range(heads)))
            send_norms(1)
            take_mem(1, 0, 2)
    for h in range(last - begin + 1, heads):
        attend(-1, memory_grads(h))
        send_mem(1, 0, h)
    for way, step, h in late:
        take_mem(way, step, h)
    if not early:
        for h in range(heads):
            take_mem(0, steps - 1, h)
            memory_gate(h)
            attend(-1, read_memory(h))
        send_norms(1)
        send_gates()
    for h in range(heads):
        add_extra(h)
    share_o[...] = jnp.broadcast_to(1.0 - share(heads - 1, size), share_o.shape)
    for h in range(heads - 1):
        take_mem(1, steps - 1, h)
        finish(h)
    for way in range(2):
        ahead = behind(1 - way)
        wait_norms(way, ahead, norm_send)
        for some in range(1, steps + 1):
            @pl.when((ahead >= 1 << (some - 1)) & ((ahead < 1 << some) | (some == steps)))
            def _():
                space = mem_src.at[way, pl.ds(0, some)]
                pltpu.make_async_copy(space, space, mem_send.at[way]).wait()
    take_mem(1, steps - 1, heads - 1)
    later_o[...] = mem_sum[1, heads - 1]
    take_norms(1)
    norm_o[...] = norm_sum[1]
    others = gate_all.at[pl.ds(0, n - 1)]
    pltpu.make_async_copy(others, others, gate_recv).wait()
    gates = gate_all[0]
    for other in range(1, n):
        gates = gates + gate_all[other]
    gate_o[...] = gates
    pltpu.make_async_copy(others, others, gate_send).wait()


def write(
    heads, size, block,
    q_ref, k_ref, v_ref, gate_ref, later_ref, norm_ref, share_ref, slope_ref, kf_ref, held_ref,
    q_hbm, k_hbm, v_hbm, gate_o, k_out, v_out, sems,
):
    rows = q_ref.shape[0]
    ready = (heads - 1) * size
    front, back = slice(0, ready), slice(ready, ready + size)
    copies = []

    def send(source, target):
        copies.append(pltpu.make_async_copy(source, target, sems.at[len(copies)]))
        copies[-1].start()

    send(q_ref, q_hbm)
    if ready:
        send(v_ref.at[:, front], v_hbm.at[:, front])
        for h in range(heads - 1):
            hs = slice(h * size, (h + 1) * size)
            for i in range(rows // block):
                here = slice(i * block, (i + 1) * block)
                k_out[here, hs] = k_ref[here, hs] + norm_ref[h:h + 1, :] * slope_ref[here, hs]
        send(k_out.at[:, front], k_hbm.at[:, front])
    high, rest = split(later_ref[...])
    beside = jnp.concatenate([high, rest], axis=1)
    below = jnp.concatenate([high, rest], axis=0)
    for i in range(rows // block):
        here = slice(i * block, (i + 1) * block)
        v_i = held_ref[0, here, back]
        low = kf_ref[here, back]
        turned = dot_nt(jnp.concatenate([v_i, v_i], axis=1), beside) + norm_ref[heads - 1:heads, :]
        k_out[here, back] = k_ref[here, back] * size ** -0.5 + turned * slope_ref[here, back]
        value = dot_nn(jnp.concatenate([low, low], axis=1), below)
        v_out[here, :] = v_ref[here, back] * share_ref[0:1, :] + value
    send(k_out.at[:, back], k_hbm.at[:, back])
    send(v_out, v_hbm.at[:, back])
    for h in range(heads):
        gate_o[h] = jnp.sum(gate_ref[h:h + 1, :])
    for copy in copies:
        copy.wait()


def solution(mesh):
    n = mesh.shape["seq"]
    longest = max(n // 2, 2)
    steps = (longest - 1).bit_length()
    reach = longest - 1

    def per_device(queries, key_vectors, value_vectors, out_grad, gate_logit, doc_index):
        rows, width = queries.shape
        heads = gate_logit.shape[0]
        size = width // heads
        block = min(256, rows)
        wide = jax.ShapeDtypeStruct((rows, width), F32)
        vmem = pl.BlockSpec(memory_space=pltpu.VMEM)
        smem = pl.BlockSpec(memory_space=pltpu.SMEM)
        hbm = pl.BlockSpec(memory_space=pltpu.HBM)
        tall = -(-heads // 8) * 8
        dma = pltpu.SemaphoreType.DMA
        small = jax.ShapeDtypeStruct((tall, size), F32)
        local = pl.pallas_call(
            functools.partial(kernel, n, steps, reach, heads, size, block),
            out_shape=(
                wide, wide, wide, small, jax.ShapeDtypeStruct((size, size), F32), small, small, wide,
                jax.ShapeDtypeStruct((rows, width), BF16), jax.ShapeDtypeStruct((3, rows, width), BF16),
            ),
            in_specs=[hbm] * 6,
            out_specs=(vmem,) * 10,
            scratch_shapes=[
                pltpu.SMEM(doc_index.shape, jnp.int32),
                pltpu.SMEM(gate_logit.shape, F32),
                pltpu.VMEM((rows, width), BF16),
                dma((4,)),
                pltpu.VMEM((rows, width), BF16),
                pltpu.VMEM((rows, width), F32),
                pltpu.VMEM((rows, width), F32),
                pltpu.VMEM((heads, rows, size), F32),
                pltpu.VMEM((3, rows, block), F32),
                pltpu.VMEM((2, rows, block), F32),
                pltpu.VMEM((heads, size, rows), BF16),
                pltpu.VMEM((tall, size), F32),
                pltpu.VMEM((n, tall, size), F32),
                pltpu.VMEM((2, tall, size), F32),
                pltpu.VMEM((2, reach, tall, size), F32),
                pltpu.VMEM((2, tall, size), F32),
                pltpu.VMEM((2, steps, heads, size, size), F32),
                pltpu.VMEM((2, steps, heads, size, size), F32),
                pltpu.VMEM((2, heads, size, size), F32),
                dma((2,)),
                dma((2,)),
                dma((2,)),
                dma((2, steps, heads)),
                dma(()),
                dma(()),
                pltpu.SemaphoreType.REGULAR((max(-(-(n - 1) // reach) - 1, 1), 2)),
            ],
            compiler_params=pltpu.CompilerParams(
                collective_id=0, has_side_effects=True, vmem_limit_bytes=40 * 1024 * 1024
            ),
            cost_estimate=pl.CostEstimate(
                flops=14 * heads * rows * rows * size, bytes_accessed=20 * rows * width,
                transcendentals=heads * rows * rows,
            ),
            name="segment_backward",
        )(*(pltpu.with_memory_space_constraint(x, pltpu.HBM) for x in (doc_index, gate_logit, queries, key_vectors, value_vectors, out_grad)))
        return pl.pallas_call(
            functools.partial(write, heads, size, block),
            out_shape=(wide, wide, wide, jax.ShapeDtypeStruct((heads,), F32)),
            in_specs=[vmem] * 10,
            out_specs=(hbm, hbm, hbm, smem),
            scratch_shapes=[pltpu.VMEM((rows, width), F32), pltpu.VMEM((rows, size), F32), dma((5,))],
            compiler_params=pltpu.CompilerParams(vmem_limit_bytes=16 * 1024 * 1024),
            cost_estimate=pl.CostEstimate(
                flops=8 * rows * width * size, bytes_accessed=12 * rows * width,
                transcendentals=rows * width,
            ),
            name="segment_finish",
        )(*local)

    spec = P("seq", "head")
    return jax.shard_map(
        per_device, mesh=mesh, in_specs=(spec, spec, spec, spec, P("head"), P()),
        out_specs=(spec, spec, spec, P("head")), check_vma=False,
    )
```
